32 devices in a mesh: dp: 2 (over x), tp: 4 (over z), pp: 4 (over y, core).
Axes of the slice: x: 2, y: 2, z: 4, core: 2. Of those that a mesh axis runs over, the one named last changes fastest.
Arguments:
- stage_buf: bfloat16 [4, 64, 512, 512], P('pp', 'dp', 'tp'), parts along dimension 1
- new_mb: bfloat16 [64, 512, 512], P('dp', 'tp'), parts along dimension 0
- positions: int32 [512], replicated
- ln_attn: float32 [4, 2, 512], P('pp')
- ln_mlp: float32 [4, 2, 512], P('pp')
- w_qkv: bfloat16 [4, 8, 3, 64, 512], P('pp', 'tp')
- w_out: bfloat16 [4, 512, 512], P('pp', 'tp')
- w_up: bfloat16 [4, 512, 2048], P('pp', None, 'tp')
- w_down: bfloat16 [4, 2048, 512], P('pp', 'tp')
Outputs:
- output 1: bfloat16 [64, 512, 512], P('dp', 'tp', 'pp'), parts along dimension 0
- output 2: bfloat16 [64, 512, 512], P('dp', 'tp', 'pp'), parts along dimension 0
- output 3: bfloat16 [4, 64, 512, 512], P('pp', 'dp', 'tp'), parts along dimension 1
There are 2 independent parts. The reference program is written for one: setup_inputs(seed, part) draws one part's arguments, and reference() takes and returns one part's arrays. A program takes and returns all parts, laid end to end along the dimension named above; an argument that names none is the same for every part.
All inputs are finite; a program needn't handle non-finite values.
Results may differ from the reference program's by a relative error of at most 0.0180202.
Values are sent between devices in bfloat16 or wider.
A program may use at most 1 GiB of HBM per device.

```python
import jax
import jax.numpy as jnp
from jax import lax

STAGES = 4
MICRO_BATCH = 32
SEQ_LEN = 512
D_MODEL = 512
N_HEADS = 8
KV_GROUPS = 8
HEAD_DIM = 64
FF_DIM = 2048
LN_EPS = 1e-5
ROPE_BASE = 10000.0


def setup_inputs(seed: int = 0, part: int = 0) -> dict:
    base_key = jax.random.key(seed)
    key_list = jax.random.split(base_key, 8)
    act_keys = jax.random.split(jax.random.fold_in(key_list[7], part), 2)
    groups = N_HEADS // KV_GROUPS
    in_scale = D_MODEL ** -0.5
    stage_buf = jax.random.normal(act_keys[0], (STAGES, MICRO_BATCH, SEQ_LEN, D_MODEL), jnp.float32).astype(jnp.bfloat16)
    new_mb = jax.random.normal(act_keys[1], (MICRO_BATCH, SEQ_LEN, D_MODEL), jnp.float32).astype(jnp.bfloat16)
    pos_steps = jax.random.randint(key_list[0], (SEQ_LEN,), 1, 4)
    offset = jax.random.randint(key_list[1], (), 0, SEQ_LEN)
    positions = (offset + jnp.cumsum(pos_steps) - 1).astype(jnp.int32)
    ln_noise = 0.2 * jax.random.normal(key_list[2], (2, STAGES, 2, D_MODEL), jnp.float32)
    ln_base = jnp.array([1.0, 0.0], jnp.float32)[None, :, None]
    w_qkv = (1.5 * in_scale * jax.random.normal(key_list[3], (STAGES, KV_GROUPS, groups + 2, HEAD_DIM, D_MODEL), jnp.float32)).astype(jnp.bfloat16)
    w_out = (in_scale * jax.random.normal(key_list[4], (STAGES, D_MODEL, D_MODEL), jnp.float32)).astype(jnp.bfloat16)
    w_up = (in_scale * jax.random.normal(key_list[5], (STAGES, D_MODEL, FF_DIM), jnp.float32)).astype(jnp.bfloat16)
    w_down = (FF_DIM ** -0.5 * jax.random.normal(key_list[6], (STAGES, FF_DIM, D_MODEL), jnp.float32)).astype(jnp.bfloat16)
    return {"stage_buf": stage_buf, "new_mb": new_mb, "positions": positions, "ln_attn": ln_base + ln_noise[0], "ln_mlp": ln_base + ln_noise[1], "w_qkv": w_qkv, "w_out": w_out, "w_up": w_up, "w_down": w_down}


def rope_tables(positions):
    inv_freq = 1.0 / (ROPE_BASE ** (jnp.arange(0, HEAD_DIM, 2).astype(jnp.float32) / HEAD_DIM))
    angles = positions.astype(jnp.float32)[:, None] * inv_freq[None, :]
    return jnp.cos(angles), jnp.sin(angles)


def layer_norm(x_in, ln_params):
    x_wide = x_in.astype(jnp.float32)
    centered = x_wide - jnp.mean(x_wide, axis=-1, keepdims=True)
    variance = jnp.mean(jnp.square(centered), axis=-1, keepdims=True)
    return (centered * lax.rsqrt(variance + LN_EPS) * ln_params[0] + ln_params[1]).astype(jnp.bfloat16)


def rotate_half(x_in, cos_tab, sin_tab):
    half_dim = x_in.shape[-1] // 2
    x_wide = x_in.astype(jnp.float32)
    first_half = x_wide[..., :half_dim]
    second_half = x_wide[..., half_dim:]
    return jnp.concatenate([first_half * cos_tab - second_half * sin_tab, second_half * cos_tab + first_half * sin_tab], axis=-1).astype(jnp.bfloat16)


def apply_layer(x_in, ln_attn, ln_mlp, w_qkv, w_out, w_up, w_down, cos_tab, sin_tab):
    groups = N_HEADS // KV_GROUPS
    a_norm = layer_norm(x_in, ln_attn).reshape(MICRO_BATCH * SEQ_LEN, D_MODEL)
    m_norm = layer_norm(x_in, ln_mlp).reshape(MICRO_BATCH * SEQ_LEN, D_MODEL)
    qkv_proj = jnp.dot(a_norm, w_qkv.reshape(-1, D_MODEL).T, preferred_element_type=jnp.float32).astype(jnp.bfloat16)
    qkv_proj = qkv_proj.reshape(MICRO_BATCH, SEQ_LEN, KV_GROUPS, groups + 2, HEAD_DIM)
    queries = rotate_half(qkv_proj[:, :, :, :groups], cos_tab[:, None, None], sin_tab[:, None, None])
    key_rot = rotate_half(qkv_proj[:, :, :, groups], cos_tab[:, None], sin_tab[:, None])
    values = qkv_proj[:, :, :, groups + 1]
    scores = jnp.einsum("bskgh,btkh->bkgst", queries.astype(jnp.float32), key_rot.astype(jnp.float32)) * HEAD_DIM ** -0.5
    causal = jnp.arange(SEQ_LEN)[:, None] >= jnp.arange(SEQ_LEN)[None, :]
    attn_probs = jax.nn.softmax(jnp.where(causal, scores, -1e30), axis=-1).astype(jnp.bfloat16)
    attn_heads = jnp.einsum("bkgst,btkh->bskgh", attn_probs.astype(jnp.float32), values.astype(jnp.float32)).astype(jnp.bfloat16)
    attn_part = jnp.dot(attn_heads.reshape(MICRO_BATCH * SEQ_LEN, D_MODEL), w_out, preferred_element_type=jnp.float32)
    hidden = jax.nn.gelu(jnp.dot(m_norm, w_up, preferred_element_type=jnp.float32), approximate=False).astype(jnp.bfloat16)
    mlp_part = jnp.dot(hidden, w_down, preferred_element_type=jnp.float32)
    summed = x_in.astype(jnp.float32) + (attn_part + mlp_part).reshape(MICRO_BATCH, SEQ_LEN, D_MODEL)
    return summed.astype(jnp.bfloat16)


def reference(stage_buf, new_mb, positions, ln_attn, ln_mlp, w_qkv, w_out, w_up, w_down):
    cos_tab, sin_tab = rope_tables(positions)

    def layer_step(stage_item):
        return apply_layer(stage_item[0], stage_item[1], stage_item[2], stage_item[3], stage_item[4], stage_item[5], stage_item[6], cos_tab, sin_tab)

    def run_tick(stage_bufs):
        return lax.map(layer_step, (stage_bufs, ln_attn, ln_mlp, w_qkv, w_out, w_up, w_down))

    out_one = run_tick(stage_buf)
    buf_one = jnp.concatenate([new_mb[None], out_one[:-1]], axis=0)
    out_two = run_tick(buf_one)
    final_buf = jnp.concatenate([jnp.zeros_like(new_mb)[None], out_two[:-1]], axis=0)
    return (out_one[-1], out_two[-1], final_buf)
```

```python
import functools

import jax
import jax.numpy as jnp
from jax import lax
from jax.experimental import pallas as pl
from jax.experimental.pallas import tpu as pltpu
from jax.sharding import PartitionSpec as P

LN_EPS = 1e-5
ROPE_BASE = 10000.0
MESH = pl.DeviceIdType.MESH
NT = (((1,), (1,)), ((), ()))
F32 = jnp.float32
BF16 = jnp.bfloat16


def rope_tables(positions, head_dim):
    inv_freq = 1.0 / (ROPE_BASE ** (jnp.arange(0, head_dim, 2).astype(F32) / head_dim))
    angles = positions.astype(F32)[:, None] * inv_freq[None, :]
    cos_tab, sin_tab = jnp.cos(angles), jnp.sin(angles)
    return jnp.concatenate([cos_tab] * 4, 1), jnp.concatenate([-sin_tab, -sin_tab, sin_tab, sin_tab], 1)


def pack_weights(w_qkv, w_out, w_up, w_down):
    heads, three, head_dim, width = w_qkv.shape
    halves = w_qkv.reshape(heads, three, 2, head_dim // 2, width)
    queries = halves[:, 0].transpose(1, 0, 2, 3).reshape(-1, width)
    keys = halves[:, 1].transpose(1, 0, 2, 3).reshape(-1, width)
    values = w_qkv[:, 2].reshape(-1, width)
    return jnp.concatenate([queries, keys, values, w_out, w_up, w_down], 0)


def layer(x_ref, w_ref, ln_ref, cos_ref, sin_ref, m_scr, q_scr, k_scr, v_scr, o_scr, acc_scr):
    seq, width = x_ref.shape
    half = seq // 2
    lane = lax.broadcasted_iota(jnp.int32, (1, 128), 1)

    def norm_rows(r, carry):
        rows = pl.ds(pl.multiple_of(r * half, half), half)
        x_wide = x_ref[rows, :].astype(F32)
        centered = x_wide - jnp.mean(x_wide, axis=-1, keepdims=True)
        variance = jnp.mean(centered * centered, axis=-1, keepdims=True)
        normed = centered * lax.rsqrt(variance + LN_EPS)
        a_norm = (normed * ln_ref[0:1, :] + ln_ref[1:2, :]).astype(BF16)
        m_scr[rows, :] = (normed * ln_ref[2:3, :] + ln_ref[3:4, :]).astype(BF16)
        cos_tab, sin_tab = cos_ref[rows, :], sin_ref[rows, :]
        for s in range(4):
            qkv = lax.dot_general(a_norm, w_ref[s, 0:384, :], NT, preferred_element_type=F32).astype(BF16)
            q_wide, k_wide = qkv[:, 0:128].astype(F32), qkv[:, 128:256].astype(F32)
            q_scr[s, rows, :] = (q_wide * cos_tab + pltpu.roll(q_wide, 64, 1) * sin_tab).astype(BF16)
            k_scr[s, rows, :] = (k_wide * cos_tab + pltpu.roll(k_wide, 64, 1) * sin_tab).astype(BF16)
            v_scr[s, rows, :] = qkv[:, 256:384]
        return carry

    lax.fori_loop(0, 2, norm_rows, 0)

    def head_pair(s, carry):
        row = lax.broadcasted_iota(jnp.int32, (half, half), 0)
        col = lax.broadcasted_iota(jnp.int32, (half, half), 1)
        causal = row >= col
        outs = [None, None]
        for hh in range(2):
            q_mask = jnp.where((lane // 32) % 2 == hh, 0.125, 0.0).astype(BF16)
            v_mask = jnp.where(lane // 64 == hh, 1.0, 0.0).astype(BF16)
            keys = [k_scr[s, 0:half, :], k_scr[s, half:seq, :]]
            vals = [v_scr[s, 0:half, :] * v_mask, v_scr[s, half:seq, :] * v_mask]
            for qb in range(2):
                q_blk = q_scr[s, qb * half:(qb + 1) * half, :] * q_mask
                scores = [lax.dot_general(q_blk, keys[kb], NT, preferred_element_type=F32) for kb in range(qb + 1)]
                scores[qb] = jnp.where(causal, scores[qb], -1e30)
                peak = functools.reduce(jnp.maximum, [jnp.max(sc, axis=-1, keepdims=True) for sc in scores])
                exps = [jnp.exp(sc - peak) for sc in scores]
                total = functools.reduce(jnp.add, [jnp.sum(e, axis=-1, keepdims=True) for e in exps])
                inv = 1.0 / total
                for kb in range(qb + 1):
                    part = jnp.dot((exps[kb] * inv).astype(BF16), vals[kb], preferred_element_type=F32)
                    outs[qb] = part if outs[qb] is None else outs[qb] + part
        for qb in range(2):
            o_scr[qb * half:(qb + 1) * half, pl.ds(pl.multiple_of(s * 128, 128), 128)] = outs[qb].astype(BF16)
        return carry

    lax.fori_loop(0, 4, head_pair, 0)

    def out_rows(r, carry):
        rows = pl.ds(pl.multiple_of(r * half, half), half)
        w_out = w_ref[:, 384:512, :].reshape(width, width)
        acc_scr[rows, :] = x_ref[rows, :].astype(F32) + jnp.dot(o_scr[rows, :], w_out, preferred_element_type=F32)
        return carry

    lax.fori_loop(0, 2, out_rows, 0)

    def mlp_part(c, carry):
        for r in range(2):
            rows = slice(r * half, (r + 1) * half)
            pre = jnp.dot(m_scr[rows, :], w_ref[c, 512:1024, :], preferred_element_type=F32)
            hidden = (0.5 * pre * (1.0 + lax.erf(pre * 0.7071067811865476))).astype(BF16)
            acc_scr[rows, :] += jnp.dot(hidden, w_ref[c, 1024:1536, :], preferred_element_type=F32)
        return carry

    lax.fori_loop(0, 4, mlp_part, 0)
    x_ref[...] = acc_scr[...].astype(BF16)


def kernel(buf_ref, mb_ref, w_loc, ln_ref, cos_ref, sin_ref, emit_one, emit_two, final,
           w_all, xs, zeros, m_scr, q_scr, k_scr, v_scr, o_scr, acc_scr,
           loc_sem, wloc_sem, xs_send, xs_recv, mb_send, mb_recv, y_recv, wz_send, wz_recv, wx_send, wx_recv,
           y_send, emit_recv, final_recv, zero_sem):
    d, t, p = lax.axis_index("dp"), lax.axis_index("tp"), lax.axis_index("pp")
    emits = (emit_one, emit_two)

    def remote(src, dst, send, recv, dp=None, tp=None, pp=None):
        where = (d if dp is None else dp, t if tp is None else tp, p if pp is None else pp)
        return pltpu.make_async_remote_copy(src, dst, send, recv, device_id=where, device_id_type=MESH)

    def wait_bytes(ref, sem):
        pltpu.make_async_copy(ref, ref, sem).wait()

    def seq_rows(rank):
        return pl.ds(pl.multiple_of(rank * 128, 128), 128)

    def x_copy(i, o):
        to = lax.rem(t + o, 4)
        return remote(buf_ref.at[0, 8 * to + i], xs.at[0, i, seq_rows(t), :], xs_send, xs_recv.at[i, o - 1], tp=to)

    def x_arrived(i, o):
        src = lax.rem(t + 4 - o, 4)
        wait_bytes(xs.at[0, i, seq_rows(src), :], xs_recv.at[i, o - 1])

    def mb_copy(i, o):
        to = lax.rem(t + o, 4)
        return remote(mb_ref.at[8 * to + i], xs.at[1, i, seq_rows(t), :], mb_send, mb_recv.at[i, o - 1], tp=to)

    def mb_arrived(i, o):
        src = lax.rem(t + 4 - o, 4)
        wait_bytes(xs.at[1, i, seq_rows(src), :], mb_recv.at[i, o - 1])

    def x_local(i):
        return pltpu.make_async_copy(buf_ref.at[0, 8 * t + i], xs.at[0, i, seq_rows(t), :], loc_sem.at[0, i])

    def mb_local(i):
        return pltpu.make_async_copy(mb_ref.at[8 * t + i], xs.at[1, i, seq_rows(t), :], loc_sem.at[1, i])

    def send_x(i):
        for o in (2, 1, 3):
            x_copy(i, o).start()

    def half_rows(dp, piece):
        size = 256 * (piece + 1)
        return pl.ds(pl.multiple_of(512 * piece + dp * size, 256), size)

    def w_copy_z(s, piece, to, slot, own):
        rows = half_rows(d, piece)
        src = w_loc.at[rows, :] if own else w_all.at[s, rows, :]
        return remote(src, w_all.at[s, rows, :], wz_send.at[slot, piece], wz_recv.at[s, piece], tp=to)

    def w_copy_x(s, piece):
        rows = half_rows(d, piece)
        return remote(w_all.at[s, rows, :], w_all.at[s, rows, :], wx_send.at[s, piece], wx_recv.at[s, piece], dp=1 - d)

    def relay(action):
        for hop in range(4):
            for piece in range(2):
                right_src, left_src = lax.max(t - hop, 0), lax.min(t + hop, 3)
                from_left, from_right = t >= hop, t + hop <= 3
                if hop:
                    for arrived, s in ((from_left, right_src), (from_right, left_src)):
                        @pl.when(arrived)
                        def _():
                            action("arrive", None, s, piece)
                if hop < 3:
                    @pl.when(jnp.logical_and(from_left, t < 3))
                    def _():
                        action("z", w_copy_z(right_src, piece, lax.min(t + 1, 3), 2 * hop, hop == 0), right_src, piece)

                    @pl.when(jnp.logical_and(from_right, t > 0))
                    def _():
                        action("z", w_copy_z(left_src, piece, lax.max(t - 1, 0), 2 * hop + 1, hop == 0), left_src, piece)
                if hop:
                    for arrived, s in ((from_left, right_src), (from_right, left_src)):
                        @pl.when(arrived)
                        def _():
                            action("x", w_copy_x(s, piece), s, piece)
            yield hop

    def start_or_wait(kind, copy, s, piece):
        if kind == "arrive":
            wait_bytes(w_all.at[s, half_rows(d, piece), :], wz_recv.at[s, piece])
        else:
            copy.start()

    def wait_sent(kind, copy, s, piece):
        if kind != "arrive":
            copy.wait_send()

    own_w = pltpu.make_async_copy(w_loc, w_all.at[t], wloc_sem)
    own_w.start()
    for hop in relay(start_or_wait):
        if hop == 0:
            for i in range(8):
                x_local(i).start()
        send_x(2 * hop)
        send_x(2 * hop + 1)

    @pl.when(p == 0)
    def _():
        def body(i, carry):
            mb_local(i).start()
            for o in (2, 1, 3):
                mb_copy(i, o).start()
            return carry
        lax.fori_loop(0, 8, body, 0)
        zeros[...] = jnp.zeros_like(zeros)

        def zero_body(i, carry):
            pltpu.make_async_copy(zeros, final.at[0, i], zero_sem).start()
            return carry
        lax.fori_loop(0, 32, zero_body, 0)

    own_w.wait()
    for o in (1, 2, 3):
        src = lax.rem(t + 4 - o, 4)
        for piece in range(2):
            wait_bytes(w_all.at[src, half_rows(1 - d, piece), :], wx_recv.at[src, piece])

    def emit_copy(tick, i, o, qq):
        to = lax.rem(t + o, 4)
        q = lax.rem(3 + qq, 4)
        src = xs.at[tick, i, seq_rows(to), seq_rows(q)]
        dst = emits[tick].at[8 * t + i]
        if o == 0 and qq == 0:
            return pltpu.make_async_copy(src, dst, emit_recv.at[tick, 0])
        return remote(src, dst, y_send.at[tick, i], emit_recv.at[tick, o], tp=to, pp=q)

    def tick_body(tick):
        def step(i, carry):
            if tick == 0:
                x_local(i).wait()
                for o in (1, 2, 3):
                    x_arrived(i, o)
            else:
                @pl.when(p == 0)
                def _():
                    mb_local(i).wait()
                    for o in (1, 2, 3):
                        mb_arrived(i, o)

                @pl.when(p > 0)
                def _():
                    wait_bytes(xs.at[1, i], y_recv.at[i])
            layer(xs.at[tick, i], w_all, ln_ref, cos_ref, sin_ref, m_scr, q_scr, k_scr, v_scr, o_scr, acc_scr)

            @pl.when(p < 3)
            def _():
                nxt = lax.min(p + 1, 3)
                if tick == 0:
                    remote(xs.at[0, i], xs.at[1, i], y_send.at[0, i], y_recv.at[i], pp=nxt).start()
                else:
                    for o in (2, 1, 3, 0):
                        to = lax.rem(t + o, 4)
                        remote(xs.at[1, i, seq_rows(to), :], final.at[0, 8 * t + i], y_send.at[1, i], final_recv.at[o],
                               tp=to, pp=nxt).start()

            @pl.when(p == 3)
            def _():
                for o in (2, 1, 3, 0):
                    for qq in (1, 2, 3, 0):
                        emit_copy(tick, i, o, qq).start()
            return carry
        lax.fori_loop(0, 8, step, 0)

    tick_body(0)
    tick_body(1)

    wait_bytes(buf_ref.at[0, 0:24], xs_send)
    for _ in relay(wait_sent):
        pass

    @pl.when(p == 0)
    def _():
        wait_bytes(mb_ref.at[0:24], mb_send)
        wait_bytes(final.at[0], zero_sem)

    @pl.when(p > 0)
    def _():
        for o in range(4):
            src = lax.rem(t + 4 - o, 4)
            wait_bytes(final.at[0, pl.ds(8 * src, 8)], final_recv.at[o])

    for tick in range(2):
        for o in range(4):
            src = lax.rem(t + 4 - o, 4)
            wait_bytes(emits[tick].at[pl.ds(8 * src, 8)], emit_recv.at[tick, o])

        def sent(i, carry):
            @pl.when(p < 3)
            def _():
                wait_bytes(xs.at[tick, i], y_send.at[tick, i])

            @pl.when(p == 3)
            def _():
                wait_bytes(emits[tick].at[0:15], y_send.at[tick, i])
            return carry
        lax.fori_loop(0, 8, sent, 0)


def solution(mesh):
    def body(stage_buf, new_mb, positions, ln_attn, ln_mlp, w_qkv, w_out, w_up, w_down):
        cos_tab, sin_tab = rope_tables(positions, w_qkv.shape[3])
        packed = pack_weights(w_qkv[0], w_out[0], w_up[0], w_down[0])
        ln_rows = jnp.concatenate([ln_attn[0], ln_mlp[0]], 0)
        batch, rows, width = new_mb.shape
        seq = 4 * rows
        emit_shape = jax.ShapeDtypeStruct((batch, rows, width // 4), BF16)
        hbm = pl.BlockSpec(memory_space=pl.ANY)
        vmem = pl.BlockSpec(memory_space=pltpu.VMEM)
        dma = pltpu.SemaphoreType.DMA
        return pl.pallas_call(
            kernel,
            out_shape=(emit_shape, emit_shape, jax.ShapeDtypeStruct(stage_buf.shape, BF16)),
            in_specs=[hbm, hbm, hbm, vmem, vmem, vmem],
            out_specs=(hbm, hbm, hbm),
            scratch_shapes=[
                pltpu.VMEM((4, 1536, width), BF16),
                pltpu.VMEM((2, batch // 4, seq, width), BF16),
                pltpu.VMEM((rows, width), BF16),
                pltpu.VMEM((seq, width), BF16),
                pltpu.VMEM((4, seq, 128), BF16),
                pltpu.VMEM((4, seq, 128), BF16),
                pltpu.VMEM((4, seq, 128), BF16),
                pltpu.VMEM((seq, width), BF16),
                pltpu.VMEM((seq, width), F32),
                dma((2, 8)), dma, dma, dma((8, 3)), dma, dma((8, 3)), dma((8,)),
                dma((6, 2)), dma((4, 2)), dma((4, 2)), dma((4, 2)),
                dma((2, 8)), dma((2, 4)), dma((4,)), dma,
            ],
            compiler_params=pltpu.CompilerParams(has_side_effects=True, vmem_limit_bytes=60 * 1024 * 1024),
            cost_estimate=pl.CostEstimate(flops=60_000_000_000, bytes_accessed=40_000_000, transcendentals=50_000_000),
        )(stage_buf, new_mb, packed, ln_rows, cos_tab, sin_tab)

    act_spec = P("dp", "tp", None)
    buf_spec = P("pp", "dp", "tp", None)
    emit_spec = P("dp", "tp", "pp")
    stack_spec = P("pp", None, None)
    return jax.shard_map(body, mesh=mesh, in_specs=(buf_spec, act_spec, P(None), stack_spec, stack_spec, P("pp", "tp", None, None, None), P("pp", "tp", None), P("pp", None, "tp"), P("pp", "tp", None)), out_specs=(emit_spec, emit_spec, buf_spec), check_vma=False)
```

```python
import functools

import jax
import jax.numpy as jnp
from jax import lax
from jax.experimental import pallas as pl
from jax.experimental.pallas import tpu as pltpu
from jax.sharding import PartitionSpec as P

LN_EPS = 1e-5
ROPE_BASE = 10000.0
MESH = pl.DeviceIdType.MESH
NT = (((1,), (1,)), ((), ()))
F32 = jnp.float32
BF16 = jnp.bfloat16


def rope_tables(positions, head_dim):
    inv_freq = 1.0 / (ROPE_BASE ** (jnp.arange(0, head_dim, 2).astype(F32) / head_dim))
    angles = positions.astype(F32)[:, None] * inv_freq[None, :]
    cos_tab, sin_tab = jnp.cos(angles), jnp.sin(angles)
    by_row = jnp.stack([jnp.concatenate([cos_tab] * 4, 1), jnp.concatenate([-sin_tab, -sin_tab, sin_tab, sin_tab], 1)])
    by_lane = jnp.stack([jnp.concatenate([cos_tab.T] * 2, 0), jnp.concatenate([sin_tab.T] * 2, 0)])
    return by_row, by_lane


def pack_weights(w_qkv, w_out, w_up, w_down):
    heads, three, head_dim, width = w_qkv.shape
    halves = w_qkv.reshape(heads, three, 2, head_dim // 2, width)
    queries = halves[:, 0].transpose(1, 0, 2, 3).reshape(-1, width)
    keys = halves[:, 1].transpose(1, 0, 2, 3).reshape(-1, width)
    values = w_qkv[:, 2].reshape(-1, width)
    return jnp.concatenate([queries, values, keys, w_out, w_up, w_down], 0)


def layer(x_ref, w_ref, ln_ref, row_ref, lane_ref, m_scr, q_scr, k_scr, v_scr, o_scr, acc_scr):
    seq, width = x_ref.shape
    half = seq // 2

    def norm_rows(r, carry):
        rows = pl.ds(pl.multiple_of(r * half, half), half)
        x_wide = x_ref[rows, :].astype(F32)
        centered = x_wide - jnp.mean(x_wide, axis=-1, keepdims=True)
        variance = jnp.mean(centered * centered, axis=-1, keepdims=True)
        normed = centered * lax.rsqrt(variance + LN_EPS)
        a_norm = (normed * ln_ref[0:1, :] + ln_ref[1:2, :]).astype(BF16)
        m_scr[rows, :] = (normed * ln_ref[2:3, :] + ln_ref[3:4, :]).astype(BF16)
        w_k = w_ref[:, 256:384, :].reshape(width, width)
        keys = lax.dot_general(a_norm, w_k, NT, preferred_element_type=F32).astype(BF16).astype(F32)
        for s in range(4):
            k_wide = keys[:, 128 * s:128 * s + 128]
            k_scr[s, rows, :] = (k_wide * row_ref[0, rows, :] + pltpu.roll(k_wide, 64, 1) * row_ref[1, rows, :]).astype(BF16)
        w_qv = w_ref[:, 0:256, :].reshape(2 * width, width)
        qv = lax.dot_general(w_qv, a_norm, NT, preferred_element_type=F32).astype(BF16)
        cos_tab, sin_tab = lane_ref[0, :, rows], lane_ref[1, :, rows]
        for s in range(4):
            first, second = qv[256 * s:256 * s + 64, :].astype(F32), qv[256 * s + 64:256 * s + 128, :].astype(F32)
            q_scr[s, 0:64, rows] = (first * cos_tab - second * sin_tab).astype(BF16)
            q_scr[s, 64:128, rows] = (second * cos_tab + first * sin_tab).astype(BF16)
            v_scr[s, :, rows] = qv[256 * s + 128:256 * s + 256, :]
        return carry

    lax.fori_loop(0, 2, norm_rows, 0)

    def head_pair(s, carry):
        causal = lax.broadcasted_iota(jnp.int32, (half, half), 0) <= lax.broadcasted_iota(jnp.int32, (half, half), 1)
        row = lax.broadcasted_iota(jnp.int32, (128, 1), 0)
        for hh in range(2):
            q_mask = jnp.where((row // 32) % 2 == hh, 0.125, 0.0).astype(BF16)
            for qb in range(2):
                cols = slice(qb * half, (qb + 1) * half)
                q_blk = q_scr[s, :, cols] * q_mask
                scores = [jnp.dot(k_scr[s, kb * half:(kb + 1) * half, :], q_blk, preferred_element_type=F32) for kb in range(qb + 1)]
                scores[qb] = jnp.where(causal, scores[qb], -1e30)
                peak = functools.reduce(jnp.maximum, [jnp.max(sc, axis=0, keepdims=True) for sc in scores])
                exps = [jnp.exp(sc - peak) for sc in scores]
                total = functools.reduce(jnp.add, [jnp.sum(e, axis=0, keepdims=True) for e in exps])
                inv = 1.0 / total
                probs = jnp.concatenate([(e * inv).astype(BF16) for e in exps], 0)
                head_out = jnp.dot(v_scr[s, 64 * hh:64 * hh + 64, 0:(qb + 1) * half], probs, preferred_element_type=F32)
                o_scr[pl.ds(pl.multiple_of(s * 128 + 64 * hh, 64), 64), cols] = head_out.astype(BF16)
        return carry

    lax.fori_loop(0, 4, head_pair, 0)

    def out_rows(r, carry):
        rows = pl.ds(pl.multiple_of(r * half, half), half)
        w_out = w_ref[:, 384:512, :].reshape(width, width)
        heads = lax.dot_general(o_scr[:, rows], w_out, (((0,), (0,)), ((), ())), preferred_element_type=F32)
        acc_scr[rows, :] = x_ref[rows, :].astype(F32) + heads
        return carry

    lax.fori_loop(0, 2, out_rows, 0)

    def mlp_part(c, carry):
        pre = jnp.dot(m_scr[...], w_ref[c, 512:1024, :], preferred_element_type=F32)
        hidden = (0.5 * pre * (1.0 + lax.erf(pre * 0.7071067811865476))).astype(BF16)
        acc_scr[...] += jnp.dot(hidden, w_ref[c, 1024:1536, :], preferred_element_type=F32)
        return carry

    lax.fori_loop(0, 4, mlp_part, 0)
    x_ref[...] = acc_scr[...].astype(BF16)


def kernel(buf_ref, mb_ref, w_loc, ln_ref, cos_ref, sin_ref, emit_one, emit_two, final,
           w_all, xs, zeros, m_scr, q_scr, k_scr, v_scr, o_scr, acc_scr,
           loc_sem, wloc_sem, xs_send, xs_recv, mb_send, mb_recv, y_recv, wz_send, wz_recv, wx_send, wx_recv,
           y_send, emit_recv, final_recv, zero_sem):
    d, t, p = lax.axis_index("dp"), lax.axis_index("tp"), lax.axis_index("pp")
    emits = (emit_one, emit_two)

    def remote(src, dst, send, recv, dp=None, tp=None, pp=None):
        where = (d if dp is None else dp, t if tp is None else tp, p if pp is None else pp)
        return pltpu.make_async_remote_copy(src, dst, send, recv, device_id=where, device_id_type=MESH)

    def wait_bytes(ref, sem):
        pltpu.make_async_copy(ref, ref, sem).wait()

    def seq_rows(rank):
        return pl.ds(pl.multiple_of(rank * 128, 128), 128)

    def x_copy(i, o):
        to = lax.rem(t + o, 4)
        return remote(buf_ref.at[0, 8 * to + i], xs.at[0, i, seq_rows(t), :], xs_send, xs_recv.at[i, o - 1], tp=to)

    def x_arrived(i, o):
        src = lax.rem(t + 4 - o, 4)
        wait_bytes(xs.at[0, i, seq_rows(src), :], xs_recv.at[i, o - 1])

    def mb_copy(i, o):
        to = lax.rem(t + o, 4)
        return remote(mb_ref.at[8 * to + i], xs.at[1, i, seq_rows(t), :], mb_send, mb_recv.at[i, o - 1], tp=to)

    def mb_arrived(i, o):
        src = lax.rem(t + 4 - o, 4)
        wait_bytes(xs.at[1, i, seq_rows(src), :], mb_recv.at[i, o - 1])

    def x_local(i):
        return pltpu.make_async_copy(buf_ref.at[0, 8 * t + i], xs.at[0, i, seq_rows(t), :], loc_sem.at[0, i])

    def mb_local(i):
        return pltpu.make_async_copy(mb_ref.at[8 * t + i], xs.at[1, i, seq_rows(t), :], loc_sem.at[1, i])

    def send_x(i):
        for o in (2, 1, 3):
            x_copy(i, o).start()

    def half_rows(dp, piece):
        size = 256 * (piece + 1)
        return pl.ds(pl.multiple_of(512 * piece + dp * size, 256), size)

    def w_copy_z(s, piece, to, slot, own):
        rows = half_rows(d, piece)
        src = w_loc.at[rows, :] if own else w_all.at[s, rows, :]
        return remote(src, w_all.at[s, rows, :], wz_send.at[slot, piece], wz_recv.at[s, piece], tp=to)

    def w_copy_x(s, piece):
        rows = half_rows(d, piece)
        return remote(w_all.at[s, rows, :], w_all.at[s, rows, :], wx_send.at[s, piece], wx_recv.at[s, piece], dp=1 - d)

    def relay(action):
        for hop in range(4):
            for piece in range(2):
                right_src, left_src = lax.max(t - hop, 0), lax.min(t + hop, 3)
                from_left, from_right = t >= hop, t + hop <= 3
                if hop:
                    for arrived, s in ((from_left, right_src), (from_right, left_src)):
                        @pl.when(arrived)
                        def _():
                            action("arrive", None, s, piece)
                if hop < 3:
                    @pl.when(jnp.logical_and(from_left, t < 3))
                    def _():
                        action("z", w_copy_z(right_src, piece, lax.min(t + 1, 3), 2 * hop, hop == 0), right_src, piece)

                    @pl.when(jnp.logical_and(from_right, t > 0))
                    def _():
                        action("z", w_copy_z(left_src, piece, lax.max(t - 1, 0), 2 * hop + 1, hop == 0), left_src, piece)
                if hop:
                    for arrived, s in ((from_left, right_src), (from_right, left_src)):
                        @pl.when(arrived)
                        def _():
                            action("x", w_copy_x(s, piece), s, piece)
            yield hop

    def start_or_wait(kind, copy, s, piece):
        if kind == "arrive":
            wait_bytes(w_all.at[s, half_rows(d, piece), :], wz_recv.at[s, piece])
        else:
            copy.start()

    def wait_sent(kind, copy, s, piece):
        if kind != "arrive":
            copy.wait_send()

    own_w = pltpu.make_async_copy(w_loc, w_all.at[t], wloc_sem)
    own_w.start()
    for hop in relay(start_or_wait):
        if hop == 0:
            for i in range(8):
                x_local(i).start()
        if hop == 3:
            for i in range(8):
                send_x(i)

    @pl.when(p == 0)
    def _():
        def body(i, carry):
            mb_local(i).start()
            for o in (2, 1, 3):
                mb_copy(i, o).start()
            return carry
        lax.fori_loop(0, 8, body, 0)
        zeros[...] = jnp.zeros_like(zeros)

        def zero_body(i, carry):
            pltpu.make_async_copy(zeros, final.at[0, i], zero_sem).start()
            return carry
        lax.fori_loop(0, 32, zero_body, 0)

    own_w.wait()
    for o in (1, 2, 3):
        src = lax.rem(t + 4 - o, 4)
        for piece in range(2):
            wait_bytes(w_all.at[src, half_rows(1 - d, piece), :], wx_recv.at[src, piece])

    def emit_copy(tick, i, o, qq):
        to = lax.rem(t + o, 4)
        q = lax.rem(3 + qq, 4)
        src = xs.at[tick, i, seq_rows(to), seq_rows(q)]
        dst = emits[tick].at[8 * t + i]
        if o == 0 and qq == 0:
            return pltpu.make_async_copy(src, dst, emit_recv.at[tick, 0])
        return remote(src, dst, y_send.at[tick, i], emit_recv.at[tick, o], tp=to, pp=q)

    def tick_body(tick):
        def step(i, carry):
            if tick == 0:
                x_local(i).wait()
                for o in (1, 2, 3):
                    x_arrived(i, o)
            else:
                @pl.when(p == 0)
                def _():
                    mb_local(i).wait()
                    for o in (1, 2, 3):
                        mb_arrived(i, o)

                @pl.when(p > 0)
                def _():
                    wait_bytes(xs.at[1, i], y_recv.at[i])
            layer(xs.at[tick, i], w_all, ln_ref, cos_ref, sin_ref, m_scr, q_scr, k_scr, v_scr, o_scr, acc_scr)

            @pl.when(p < 3)
            def _():
                nxt = lax.min(p + 1, 3)
                if tick == 0:
                    remote(xs.at[0, i], xs.at[1, i], y_send.at[0, i], y_recv.at[i], pp=nxt).start()
                else:
                    for o in (2, 1, 3, 0):
                        to = lax.rem(t + o, 4)
                        remote(xs.at[1, i, seq_rows(to), :], final.at[0, 8 * t + i], y_send.at[1, i], final_recv.at[o],
                               tp=to, pp=nxt).start()

            @pl.when(p == 3)
            def _():
                for o in (2, 1, 3, 0):
                    for qq in (1, 2, 3, 0):
                        emit_copy(tick, i, o, qq).start()
            return carry
        lax.fori_loop(0, 8, step, 0)

    tick_body(0)
    tick_body(1)

    wait_bytes(buf_ref.at[0, 0:24], xs_send)
    for _ in relay(wait_sent):
        pass

    @pl.when(p == 0)
    def _():
        wait_bytes(mb_ref.at[0:24], mb_send)
        wait_bytes(final.at[0], zero_sem)

    @pl.when(p > 0)
    def _():
        for o in range(4):
            src = lax.rem(t + 4 - o, 4)
            wait_bytes(final.at[0, pl.ds(8 * src, 8)], final_recv.at[o])

    for tick in range(2):
        for o in range(4):
            src = lax.rem(t + 4 - o, 4)
            wait_bytes(emits[tick].at[pl.ds(8 * src, 8)], emit_recv.at[tick, o])

        def sent(i, carry):
            @pl.when(p < 3)
            def _():
                wait_bytes(xs.at[tick, i], y_send.at[tick, i])

            @pl.when(p == 3)
            def _():
                wait_bytes(emits[tick].at[0:15], y_send.at[tick, i])
            return carry
        lax.fori_loop(0, 8, sent, 0)


def solution(mesh):
    def body(stage_buf, new_mb, positions, ln_attn, ln_mlp, w_qkv, w_out, w_up, w_down):
        cos_tab, sin_tab = rope_tables(positions, w_qkv.shape[3])
        packed = pack_weights(w_qkv[0], w_out[0], w_up[0], w_down[0])
        ln_rows = jnp.concatenate([ln_attn[0], ln_mlp[0]], 0)
        batch, rows, width = new_mb.shape
        seq = 4 * rows
        emit_shape = jax.ShapeDtypeStruct((batch, rows, width // 4), BF16)
        hbm = pl.BlockSpec(memory_space=pl.ANY)
        vmem = pl.BlockSpec(memory_space=pltpu.VMEM)
        dma = pltpu.SemaphoreType.DMA
        return pl.pallas_call(
            kernel,
            out_shape=(emit_shape, emit_shape, jax.ShapeDtypeStruct(stage_buf.shape, BF16)),
            in_specs=[hbm, hbm, hbm, vmem, vmem, vmem],
            out_specs=(hbm, hbm, hbm),
            scratch_shapes=[
                pltpu.VMEM((4, 1536, width), BF16),
                pltpu.VMEM((2, batch // 4, seq, width), BF16),
                pltpu.VMEM((rows, width), BF16),
                pltpu.VMEM((seq, width), BF16),
                pltpu.VMEM((4, 128, seq), BF16),
                pltpu.VMEM((4, seq, 128), BF16),
                pltpu.VMEM((4, 128, seq), BF16),
                pltpu.VMEM((seq, width), BF16),
                pltpu.VMEM((seq, width), F32),
                dma((2, 8)), dma, dma, dma((8, 3)), dma, dma((8, 3)), dma((8,)),
                dma((6, 2)), dma((4, 2)), dma((4, 2)), dma((4, 2)),
                dma((2, 8)), dma((2, 4)), dma((4,)), dma,
            ],
            compiler_params=pltpu.CompilerParams(has_side_effects=True, vmem_limit_bytes=60 * 1024 * 1024),
            cost_estimate=pl.CostEstimate(flops=60_000_000_000, bytes_accessed=40_000_000, transcendentals=50_000_000),
        )(stage_buf, new_mb, packed, ln_rows, cos_tab, sin_tab)

    act_spec = P("dp", "tp", None)
    buf_spec = P("pp", "dp", "tp", None)
    emit_spec = P("dp", "tp", "pp")
    stack_spec = P("pp", None, None)
    return jax.shard_map(body, mesh=mesh, in_specs=(buf_spec, act_spec, P(None), stack_spec, stack_spec, P("pp", "tp", None, None, None), P("pp", "tp", None), P("pp", None, "tp"), P("pp", "tp", None)), out_specs=(emit_spec, emit_spec, buf_spec), check_vma=False)
```

```python
import functools

import jax
import jax.numpy as jnp
import numpy as np
from jax import lax
from jax.experimental import pallas as pl
from jax.experimental.pallas import tpu as pltpu
from jax.sharding import PartitionSpec as P

LN_EPS = 1e-5
ROPE_BASE = 10000.0
MESH = pl.DeviceIdType.MESH
NT = (((1,), (1,)), ((), ()))
F32 = jnp.float32
BF16 = jnp.bfloat16


def rope_angles(positions, inv_freq):
    seq = positions.shape[1]
    by_row = jnp.broadcast_to(positions.astype(F32), (128, seq)).T * inv_freq
    sign = jnp.where(lax.broadcasted_iota(jnp.int32, (1, 128), 1) < 64, -1.0, 1.0)
    cos_tab, sin_tab = jnp.cos(by_row), jnp.sin(by_row)
    return cos_tab, sin_tab * sign, cos_tab.T[64:128, :], sin_tab.T[64:128, :]


def layer(x_ref, w_ref, ln_ref, row_ref, lane_ref, m_scr, q_scr, k_scr, v_scr, o_scr, acc_scr):
    seq, width = x_ref.shape
    half = seq // 2

    def norm_rows(r, carry):
        rows = pl.ds(pl.multiple_of(r * half, half), half)
        x_wide = x_ref[rows, :].astype(F32)
        acc_scr[rows, :] = x_wide
        centered = x_wide - jnp.mean(x_wide, axis=-1, keepdims=True)
        variance = jnp.mean(centered * centered, axis=-1, keepdims=True)
        normed = centered * lax.rsqrt(variance + LN_EPS)
        a_norm = (normed * ln_ref[0, 0:1, :] + ln_ref[0, 1:2, :]).astype(BF16)
        m_scr[rows, :] = (normed * ln_ref[1, 0:1, :] + ln_ref[1, 1:2, :]).astype(BF16)
        w_k = w_ref[:, 256:384, :].reshape(width, width)
        keys = lax.dot_general(a_norm, w_k, NT, preferred_element_type=F32).astype(BF16).astype(F32)
        for s in range(4):
            k_wide = keys[:, 128 * s:128 * s + 128]
            k_scr[s, rows, :] = (k_wide * row_ref[0, rows, :] + pltpu.roll(k_wide, 64, 1) * row_ref[1, rows, :]).astype(BF16)
        w_qv = w_ref[:, 0:256, :].reshape(2 * width, width)
        qv = lax.dot_general(w_qv, a_norm, NT, preferred_element_type=F32).astype(BF16)
        cos_tab, sin_tab = lane_ref[0, :, rows], lane_ref[1, :, rows]
        for s in range(4):
            first, second = qv[256 * s:256 * s + 64, :].astype(F32), qv[256 * s + 64:256 * s + 128, :].astype(F32)
            q_scr[s, 0:64, rows] = (first * cos_tab - second * sin_tab).astype(BF16)
            q_scr[s, 64:128, rows] = (second * cos_tab + first * sin_tab).astype(BF16)
            v_scr[s, :, rows] = qv[256 * s + 128:256 * s + 256, :]
        return carry

    lax.fori_loop(0, 2, norm_rows, 0, unroll=2)

    def head_pair_and_mlp_part(s, carry):
        pre = jnp.dot(m_scr[...], w_ref[s, 512:1024, :], preferred_element_type=F32)
        causal = lax.broadcasted_iota(jnp.int32, (half, half), 0) <= lax.broadcasted_iota(jnp.int32, (half, half), 1)
        row = lax.broadcasted_iota(jnp.int32, (128, 1), 0)
        for hh in range(2):
            q_mask = jnp.where((row // 32) % 2 == hh, 0.125, 0.0).astype(BF16)
            for qb in range(2):
                cols = slice(qb * half, (qb + 1) * half)
                q_blk = q_scr[s, :, cols] * q_mask
                scores = [jnp.dot(k_scr[s, kb * half:(kb + 1) * half, :], q_blk, preferred_element_type=F32) for kb in range(qb + 1)]
                scores[qb] = jnp.where(causal, scores[qb], -1e30)
                peak = functools.reduce(jnp.maximum, [jnp.max(sc, axis=0, keepdims=True) for sc in scores])
                exps = [jnp.exp(sc - peak) for sc in scores]
                total = functools.reduce(jnp.add, [jnp.sum(e, axis=0, keepdims=True) for e in exps])
                probs = jnp.concatenate([e.astype(BF16) for e in exps], 0)
                head_out = jnp.dot(v_scr[s, 64 * hh:64 * hh + 64, 0:(qb + 1) * half], probs, preferred_element_type=F32)
                o_scr[pl.ds(pl.multiple_of(s * 128 + 64 * hh, 64), 64), cols] = (head_out * (1.0 / total)).astype(BF16)
        hidden = (0.5 * pre * (1.0 + lax.erf(pre * 0.7071067811865476))).astype(BF16)
        acc_scr[...] += jnp.dot(hidden, w_ref[s, 1024:1536, :], preferred_element_type=F32)
        return carry

    lax.fori_loop(0, 4, head_pair_and_mlp_part, 0, unroll=4)

    def out_rows(r, carry):
        rows = pl.ds(pl.multiple_of(r * half, half), half)
        w_out = w_ref[:, 384:512, :].reshape(width, width)
        heads = lax.dot_general(o_scr[:, rows], w_out, (((0,), (0,)), ((), ())), preferred_element_type=F32)
        x_ref[rows, :] = (acc_scr[rows, :] + heads).astype(BF16)
        return carry

    lax.fori_loop(0, 2, out_rows, 0, unroll=2)


def kernel(buf_ref, mb_ref, pos_ref, freq_ref, ln_attn, ln_mlp, w_qkv, w_out, w_up, w_down, emit_one, emit_two, final,
           w_all, xs, ln_scr, row_scr, lane_scr, m_scr, q_scr, k_scr, v_scr, o_scr, acc_scr,
           loc_sem, wloc_sem, ln_sem, xs_send, xs_recv, mb_send, mb_recv, y_recv, wz_send, wz_recv, wx_send, wx_recv,
           y_send, emit_recv, final_recv):
    d, t, p = lax.axis_index("dp"), lax.axis_index("tp"), lax.axis_index("pp")
    emits = (emit_one, emit_two)

    def remote(src, dst, send, recv, dp=None, tp=None, pp=None):
        where = (d if dp is None else dp, t if tp is None else tp, p if pp is None else pp)
        return pltpu.make_async_remote_copy(src, dst, send, recv, device_id=where, device_id_type=MESH)

    def wait_bytes(ref, sem):
        pltpu.make_async_copy(ref, ref, sem).wait()

    def seq_rows(rank):
        return pl.ds(pl.multiple_of(rank * 128, 128), 128)

    def x_copy(i, o):
        to = lax.rem(t + o, 4)
        return remote(buf_ref.at[0, 8 * to + i], xs.at[0, i, seq_rows(t), :], xs_send, xs_recv.at[i, o - 1], tp=to)

    def x_arrived(i, o):
        src = lax.rem(t + 4 - o, 4)
        wait_bytes(xs.at[0, i, seq_rows(src), :], xs_recv.at[i, o - 1])

    def mb_copy(i, o):
        to = lax.rem(t + o, 4)
        return remote(mb_ref.at[8 * to + i], xs.at[1, i, seq_rows(t), :], mb_send, mb_recv.at[i, o - 1], tp=to)

    def mb_arrived(i, o):
        src = lax.rem(t + 4 - o, 4)
        wait_bytes(xs.at[1, i, seq_rows(src), :], mb_recv.at[i, o - 1])

    def x_local(i):
        return pltpu.make_async_copy(buf_ref.at[0, 8 * t + i], xs.at[0, i, seq_rows(t), :], loc_sem.at[0, i])

    def mb_local(i):
        return pltpu.make_async_copy(mb_ref.at[8 * t + i], xs.at[1, i, seq_rows(t), :], loc_sem.at[1, i])

    def send_x(i):
        for o in (2, 1, 3):
            x_copy(i, o).start()

    def half_rows(dp, piece):
        size = 256 * (piece + 1)
        return pl.ds(pl.multiple_of(512 * piece + dp * size, 256), size)

    def w_copy_z(s, piece, to, slot):
        rows = half_rows(d, piece)
        return remote(w_all.at[s, rows, :], w_all.at[s, rows, :], wz_send.at[slot, piece], wz_recv.at[s, piece], tp=to)

    def w_copy_x(s, piece):
        rows = half_rows(d, piece)
        return remote(w_all.at[s, rows, :], w_all.at[s, rows, :], wx_send.at[s, piece], wx_recv.at[s, piece], dp=1 - d)

    def relay(action):
        for hop in range(4):
            for piece in range(2):
                right_src, left_src = lax.max(t - hop, 0), lax.min(t + hop, 3)
                from_left, from_right = t >= hop, t + hop <= 3
                if hop:
                    for arrived, s in ((from_left, right_src), (from_right, left_src)):
                        @pl.when(arrived)
                        def _():
                            action("arrive", None, s, piece)
                if hop < 3:
                    @pl.when(jnp.logical_and(from_left, t < 3))
                    def _():
                        action("z", w_copy_z(right_src, piece, lax.min(t + 1, 3), 2 * hop), right_src, piece)

                    @pl.when(jnp.logical_and(from_right, t > 0))
                    def _():
                        action("z", w_copy_z(left_src, piece, lax.max(t - 1, 0), 2 * hop + 1), left_src, piece)
                if hop:
                    for arrived, s in ((from_left, right_src), (from_right, left_src)):
                        @pl.when(arrived)
                        def _():
                            action("x", w_copy_x(s, piece), s, piece)
            yield hop

    def start_or_wait(kind, copy, s, piece):
        if kind == "arrive":
            wait_bytes(w_all.at[s, half_rows(d, piece), :], wz_recv.at[s, piece])
        else:
            copy.start()

    def wait_sent(kind, copy, s, piece):
        if kind != "arrive":
            copy.wait_send()

    own = []
    for head in range(2):
        for j, row in ((0, 0), (1, 256)):
            for side in range(2):
                own.append((w_qkv.at[0, head, j, pl.ds(32 * side, 32), :], row + 64 * side + 32 * head, 32))
        own.append((w_qkv.at[0, head, 2], 128 + 64 * head, 64))
    own += [(w_out.at[0], 384, 128), (w_up.at[0], 512, 512), (w_down.at[0], 1024, 512)]
    for src, row, size in own:
        pltpu.make_async_copy(src, w_all.at[t, pl.ds(row, size), :], wloc_sem).start()
    small = [pltpu.make_async_copy(ln_attn.at[0], ln_scr.at[0], ln_sem.at[0]), pltpu.make_async_copy(ln_mlp.at[0], ln_scr.at[1], ln_sem.at[1])]
    for copy in small:
        copy.start()
    send_x(0)
    wait_bytes(w_all.at[t], wloc_sem)
    for hop in relay(start_or_wait):
        if hop == 0:
            for i in range(8):
                x_local(i).start()
        for i in ((), (1, 2), (3, 4), (5, 6, 7))[hop]:
            send_x(i)

    @pl.when(p == 0)
    def _():
        def body(i, carry):
            mb_local(i).start()
            for o in (2, 1, 3):
                mb_copy(i, o).start()
            return carry
        lax.fori_loop(0, 8, body, 0)

        def zero_body(i, carry):
            final[0, i] = jnp.zeros(final.shape[2:], BF16)
            return carry
        lax.fori_loop(0, 32, zero_body, 0)

    for copy in small:
        copy.wait()
    row_scr[0], row_scr[1], lane_scr[0], lane_scr[1] = rope_angles(pos_ref[...], freq_ref[...])
    for o in (1, 2, 3):
        src = lax.rem(t + 4 - o, 4)
        for piece in range(2):
            wait_bytes(w_all.at[src, half_rows(1 - d, piece), :], wx_recv.at[src, piece])

    def emit_copy(tick, i, o, qq):
        to = lax.rem(t + o, 4)
        q = lax.rem(3 + qq, 4)
        src = xs.at[tick, i, seq_rows(to), seq_rows(q)]
        dst = emits[tick].at[8 * t + i]
        return remote(src, dst, y_send.at[tick, i], emit_recv.at[tick, o], tp=to, pp=q)

    def tick_body(tick):
        def step(i, carry):
            if tick == 0:
                x_local(i).wait()
                for o in (1, 2, 3):
                    x_arrived(i, o)
            else:
                @pl.when(p == 0)
                def _():
                    mb_local(i).wait()
                    for o in (1, 2, 3):
                        mb_arrived(i, o)

                @pl.when(p > 0)
                def _():
                    wait_bytes(xs.at[1, i], y_recv.at[i])
            layer(xs.at[tick, i], w_all, ln_scr, row_scr, lane_scr, m_scr, q_scr, k_scr, v_scr, o_scr, acc_scr)

            @pl.when(p < 3)
            def _():
                nxt = lax.min(p + 1, 3)
                if tick == 0:
                    remote(xs.at[0, i], xs.at[1, i], y_send.at[0, i], y_recv.at[i], pp=nxt).start()
                else:
                    for o in (2, 1, 3, 0):
                        to = lax.rem(t + o, 4)
                        remote(xs.at[1, i, seq_rows(to), :], final.at[0, 8 * t + i], y_send.at[1, i], final_recv.at[o],
                               tp=to, pp=nxt).start()

            @pl.when(p == 3)
            def _():
                for o in (2, 1, 3, 0):
                    for qq in (1, 2, 3, 0):
                        if o == 0 and qq == 0:
                            emits[tick][8 * t + i] = xs[tick, i, seq_rows(t), 384:512]
                        else:
                            emit_copy(tick, i, o, qq).start()
            return carry
        lax.fori_loop(0, 8, step, 0)

    tick_body(0)
    tick_body(1)

    wait_bytes(buf_ref.at[0, 0:24], xs_send)
    for _ in relay(wait_sent):
        pass

    @pl.when(p == 0)
    def _():
        wait_bytes(mb_ref.at[0:24], mb_send)

    @pl.when(p > 0)
    def _():
        for o in range(4):
            src = lax.rem(t + 4 - o, 4)
            wait_bytes(final.at[0, pl.ds(8 * src, 8)], final_recv.at[o])

    for tick in range(2):
        for o in range(4):
            @pl.when(jnp.logical_or(p < 3, o > 0))
            def _():
                wait_bytes(emits[tick].at[pl.ds(8 * lax.rem(t + 4 - o, 4), 8)], emit_recv.at[tick, o])

        def sent(i, carry):
            @pl.when(p < 3)
            def _():
                wait_bytes(xs.at[tick, i], y_send.at[tick, i])

            @pl.when(p == 3)
            def _():
                wait_bytes(emits[tick].at[0:15], y_send.at[tick, i])
            return carry
        lax.fori_loop(0, 8, sent, 0)


def solution(mesh):
    def body(stage_buf, new_mb, positions, ln_attn, ln_mlp, w_qkv, w_out, w_up, w_down):
        head_dim = w_qkv.shape[3]
        inv_freq = 1.0 / np.power(np.float32(ROPE_BASE), np.arange(0, head_dim, 2).astype(np.float32) / np.float32(head_dim))
        inv_freq = jnp.asarray(np.tile(inv_freq.astype(np.float32), 4)[None])
        batch, rows, width = new_mb.shape
        seq = 4 * rows
        emit_shape = jax.ShapeDtypeStruct((batch, rows, width // 4), BF16)
        hbm = pl.BlockSpec(memory_space=pl.ANY)
        vmem = pl.BlockSpec(memory_space=pltpu.VMEM)
        dma = pltpu.SemaphoreType.DMA
        shapes = (emit_shape, emit_shape, jax.ShapeDtypeStruct(stage_buf.shape, BF16))
        return pl.pallas_call(
            kernel,
            out_shape=tuple(pltpu.VMEM(sh.shape, BF16) for sh in shapes),
            in_specs=[hbm, hbm, vmem, vmem, hbm, hbm, hbm, hbm, hbm, hbm],
            out_specs=(vmem, vmem, vmem),
            scratch_shapes=[
                pltpu.VMEM((4, 1536, width), BF16),
                pltpu.VMEM((2, batch // 4, seq, width), BF16),
                pltpu.VMEM((2, 2, width), F32),
                pltpu.VMEM((2, seq, 128), F32),
                pltpu.VMEM((2, 64, seq), F32),
                pltpu.VMEM((seq, width), BF16),
                pltpu.VMEM((4, 128, seq), BF16),
                pltpu.VMEM((4, seq, 128), BF16),
                pltpu.VMEM((4, 128, seq), BF16),
                pltpu.VMEM((seq, width), BF16),
                pltpu.VMEM((seq, width), F32),
                dma((2, 8)), dma, dma((2,)), dma, dma((8, 3)), dma, dma((8, 3)), dma((8,)),
                dma((6, 2)), dma((4, 2)), dma((4, 2)), dma((4, 2)),
                dma((2, 8)), dma((2, 4)), dma((4,)),
            ],
            compiler_params=pltpu.CompilerParams(has_side_effects=True, vmem_limit_bytes=57 * 1024 * 1024),
            cost_estimate=pl.CostEstimate(flops=60_000_000_000, bytes_accessed=40_000_000, transcendentals=50_000_000),
        )(stage_buf, new_mb, positions[None, :], inv_freq, ln_attn, ln_mlp, w_qkv, w_out, w_up, w_down)

    act_spec = P("dp", "tp", None)
    buf_spec = P("pp", "dp", "tp", None)
    emit_spec = P("dp", "tp", "pp")
    stack_spec = P("pp", None, None)
    return jax.shard_map(body, mesh=mesh, in_specs=(buf_spec, act_spec, P(None), stack_spec, stack_spec, P("pp", "tp", None, None, None), P("pp", "tp", None), P("pp", None, "tp"), P("pp", "tp", None)), out_specs=(emit_spec, emit_spec, buf_spec), check_vma=False)
```

```python
import functools

import jax
import jax.numpy as jnp
import numpy as np
from jax import lax
from jax.experimental import pallas as pl
from jax.experimental.pallas import tpu as pltpu
from jax.sharding import PartitionSpec as P

LN_EPS = 1e-5
ROPE_BASE = 10000.0
MESH = pl.DeviceIdType.MESH
NT = (((1,), (1,)), ((), ()))
F32 = jnp.float32
BF16 = jnp.bfloat16


def rope_angles(positions, inv_freq):
    seq = positions.shape[1]
    by_row = jnp.broadcast_to(positions.astype(F32), (128, seq)).T * inv_freq
    sign = jnp.where(lax.broadcasted_iota(jnp.int32, (1, 128), 1) < 64, -1.0, 1.0)
    cos_tab, sin_tab = jnp.cos(by_row), jnp.sin(by_row)
    return cos_tab, sin_tab * sign, cos_tab.T[64:128, :], sin_tab.T[64:128, :]


def layer(x_ref, w_ref, ln_ref, row_ref, lane_ref, m_scr, q_scr, k_scr, v_scr, o_scr, acc_scr):
    seq, width = x_ref.shape
    half = seq // 2

    def norm_rows(r, carry):
        rows = pl.ds(pl.multiple_of(r * half, half), half)
        x_wide = x_ref[rows, :].astype(F32)
        acc_scr[rows, :] = x_wide
        centered = x_wide - jnp.mean(x_wide, axis=-1, keepdims=True)
        variance = jnp.mean(centered * centered, axis=-1, keepdims=True)
        normed = centered * lax.rsqrt(variance + LN_EPS)
        a_norm = (normed * ln_ref[0, 0:1, :] + ln_ref[0, 1:2, :]).astype(BF16)
        m_scr[rows, :] = (normed * ln_ref[1, 0:1, :] + ln_ref[1, 1:2, :]).astype(BF16)
        w_k = w_ref[:, 256:384, :].reshape(width, width)
        keys = lax.dot_general(a_norm, w_k, NT, preferred_element_type=F32).astype(BF16).astype(F32)
        for s in range(4):
            k_wide = keys[:, 128 * s:128 * s + 128]
            k_scr[s, rows, :] = (k_wide * row_ref[0, rows, :] + pltpu.roll(k_wide, 64, 1) * row_ref[1, rows, :]).astype(BF16)
        w_qv = w_ref[:, 0:256, :].reshape(2 * width, width)
        qv = lax.dot_general(w_qv, a_norm, NT, preferred_element_type=F32).astype(BF16)
        cos_tab, sin_tab = lane_ref[0, :, rows], lane_ref[1, :, rows]
        for s in range(4):
            first, second = qv[256 * s:256 * s + 64, :].astype(F32), qv[256 * s + 64:256 * s + 128, :].astype(F32)
            q_scr[s, 0:64, rows] = (first * cos_tab - second * sin_tab).astype(BF16)
            q_scr[s, 64:128, rows] = (second * cos_tab + first * sin_tab).astype(BF16)
            v_scr[s, :, rows] = qv[256 * s + 128:256 * s + 256, :]
        return carry

    lax.fori_loop(0, 2, norm_rows, 0, unroll=2)

    def head_pair_and_mlp_part(s, carry):
        pre = jnp.dot(m_scr[...], w_ref[s, 512:1024, :], preferred_element_type=F32)
        causal = lax.broadcasted_iota(jnp.int32, (half, half), 0) <= lax.broadcasted_iota(jnp.int32, (half, half), 1)
        row = lax.broadcasted_iota(jnp.int32, (128, 1), 0)
        for hh in range(2):
            q_mask = jnp.where((row // 32) % 2 == hh, 0.125, 0.0).astype(BF16)
            for qb in range(2):
                cols = slice(qb * half, (qb + 1) * half)
                q_blk = q_scr[s, :, cols] * q_mask
                scores = [jnp.dot(k_scr[s, kb * half:(kb + 1) * half, :], q_blk, preferred_element_type=F32) for kb in range(qb + 1)]
                scores[qb] = jnp.where(causal, scores[qb], -1e30)
                peak = functools.reduce(jnp.maximum, [jnp.max(sc, axis=0, keepdims=True) for sc in scores])
                exps = [jnp.exp(sc - peak) for sc in scores]
                total = functools.reduce(jnp.add, [jnp.sum(e, axis=0, keepdims=True) for e in exps])
                probs = jnp.concatenate([e.astype(BF16) for e in exps], 0)
                head_out = jnp.dot(v_scr[s, 64 * hh:64 * hh + 64, 0:(qb + 1) * half], probs, preferred_element_type=F32)
                o_scr[pl.ds(pl.multiple_of(s * 128 + 64 * hh, 64), 64), cols] = (head_out * (1.0 / total)).astype(BF16)
        hidden = (0.5 * pre * (1.0 + lax.erf(pre * 0.7071067811865476))).astype(BF16)
        acc_scr[...] += jnp.dot(hidden, w_ref[s, 1024:1536, :], preferred_element_type=F32)
        return carry

    lax.fori_loop(0, 4, head_pair_and_mlp_part, 0, unroll=4)

    def out_rows(r, carry):
        rows = pl.ds(pl.multiple_of(r * half, half), half)
        w_out = w_ref[:, 384:512, :].reshape(width, width)
        heads = lax.dot_general(o_scr[:, rows], w_out, (((0,), (0,)), ((), ())), preferred_element_type=F32)
        x_ref[rows, :] = (acc_scr[rows, :] + heads).astype(BF16)
        return carry

    lax.fori_loop(0, 2, out_rows, 0, unroll=2)


def kernel(buf_ref, mb_ref, pos_ref, freq_ref, ln_attn, ln_mlp, w_qkv, w_out, w_up, w_down, emit_one, emit_two, final,
           w_all, xs, ln_scr, row_scr, lane_scr, m_scr, q_scr, k_scr, v_scr, o_scr, acc_scr,
           loc_sem, wloc_sem, ln_sem, xs_send, xs_recv, mb_send, mb_recv, y_recv, wz_send, wz_recv, wx_send, wx_recv,
           y_send, emit_recv, final_recv):
    d, t, p = lax.axis_index("dp"), lax.axis_index("tp"), lax.axis_index("pp")
    emits = (emit_one, emit_two)

    def remote(src, dst, send, recv, dp=None, tp=None, pp=None):
        where = (d if dp is None else dp, t if tp is None else tp, p if pp is None else pp)
        return pltpu.make_async_remote_copy(src, dst, send, recv, device_id=where, device_id_type=MESH)

    def wait_bytes(ref, sem):
        pltpu.make_async_copy(ref, ref, sem).wait()

    def seq_rows(rank):
        return pl.ds(pl.multiple_of(rank * 128, 128), 128)

    def x_copy(i, o):
        to = lax.rem(t + o, 4)
        return remote(buf_ref.at[0, 8 * to + i], xs.at[0, i, seq_rows(t), :], xs_send, xs_recv.at[i, o - 1], tp=to)

    def x_arrived(i, o):
        src = lax.rem(t + 4 - o, 4)
        wait_bytes(xs.at[0, i, seq_rows(src), :], xs_recv.at[i, o - 1])

    def mb_copy(i, o):
        to = lax.rem(t + o, 4)
        return remote(mb_ref.at[8 * to + i], xs.at[1, i, seq_rows(t), :], mb_send, mb_recv.at[i, o - 1], tp=to)

    def mb_arrived(i, o):
        src = lax.rem(t + 4 - o, 4)
        wait_bytes(xs.at[1, i, seq_rows(src), :], mb_recv.at[i, o - 1])

    def x_local(i):
        return pltpu.make_async_copy(buf_ref.at[0, 8 * t + i], xs.at[0, i, seq_rows(t), :], loc_sem.at[0, i])

    def mb_local(i):
        return pltpu.make_async_copy(mb_ref.at[8 * t + i], xs.at[1, i, seq_rows(t), :], loc_sem.at[1, i])

    def send_x(i):
        for o in (2, 1, 3):
            x_copy(i, o).start()

    def half_rows(dp, piece):
        size = 256 * (piece + 1)
        return pl.ds(pl.multiple_of(512 * piece + dp * size, 256), size)

    def w_copy_z(s, piece, to, slot):
        rows = half_rows(d, piece)
        return remote(w_all.at[s, rows, :], w_all.at[s, rows, :], wz_send.at[slot, piece], wz_recv.at[s, piece], tp=to)

    def w_copy_x(s, piece):
        rows = half_rows(d, piece)
        return remote(w_all.at[s, rows, :], w_all.at[s, rows, :], wx_send.at[s, piece], wx_recv.at[s, piece], dp=1 - d)

    def relay(action):
        for hop in range(4):
            for piece in range(2):
                right_src, left_src = lax.max(t - hop, 0), lax.min(t + hop, 3)
                from_left, from_right = t >= hop, t + hop <= 3
                if hop:
                    for arrived, s in ((from_left, right_src), (from_right, left_src)):
                        @pl.when(arrived)
                        def _():
                            action("arrive", None, s, piece)
                if hop < 3:
                    @pl.when(jnp.logical_and(from_left, t < 3))
                    def _():
                        action("z", w_copy_z(right_src, piece, lax.min(t + 1, 3), 2 * hop), right_src, piece)

                    @pl.when(jnp.logical_and(from_right, t > 0))
                    def _():
                        action("z", w_copy_z(left_src, piece, lax.max(t - 1, 0), 2 * hop + 1), left_src, piece)
                if hop:
                    for arrived, s in ((from_left, right_src), (from_right, left_src)):
                        @pl.when(arrived)
                        def _():
                            action("x", w_copy_x(s, piece), s, piece)
            yield hop

    def start_or_wait(kind, copy, s, piece):
        if kind == "arrive":
            wait_bytes(w_all.at[s, half_rows(d, piece), :], wz_recv.at[s, piece])
        else:
            copy.start()

    def wait_sent(kind, copy, s, piece):
        if kind != "arrive":
            copy.wait_send()

    own = []
    for head in range(2):
        for j, row in ((0, 0), (1, 256)):
            for side in range(2):
                own.append((w_qkv.at[0, head, j, pl.ds(32 * side, 32), :], row + 64 * side + 32 * head, 32))
        own.append((w_qkv.at[0, head, 2], 128 + 64 * head, 64))
    own += [(w_out.at[0], 384, 128), (w_up.at[0], 512, 512), (w_down.at[0], 1024, 512)]
    for src, row, size in own:
        pltpu.make_async_copy(src, w_all.at[t, pl.ds(row, size), :], wloc_sem).start()
    small = [pltpu.make_async_copy(ln_attn.at[0], ln_scr.at[0], ln_sem.at[0]), pltpu.make_async_copy(ln_mlp.at[0], ln_scr.at[1], ln_sem.at[1])]
    for copy in small:
        copy.start()
    for i in range(8):
        x_local(i).start()

    barrier = pltpu.get_barrier_semaphore()
    for o in range(4):
        for oo in range(4):
            if o or oo:
                where = (d, lax.rem(t + o, 4), lax.rem(p + oo, 4))
                pl.semaphore_signal(barrier, inc=1, device_id=where, device_id_type=MESH)
    pl.semaphore_signal(barrier, inc=1, device_id=(1 - d, t, p), device_id_type=MESH)
    pl.semaphore_wait(barrier, 16)

    send_x(0)
    wait_bytes(w_all.at[t], wloc_sem)
    for hop in relay(start_or_wait):
        for i in ((), (1, 2), (3, 4), (5, 6, 7))[hop]:
            send_x(i)

    @pl.when(p == 0)
    def _():
        def body(i, carry):
            mb_local(i).start()
            for o in (2, 1, 3):
                mb_copy(i, o).start()
            return carry
        lax.fori_loop(0, 8, body, 0)

        def zero_body(i, carry):
            final[0, i] = jnp.zeros(final.shape[2:], BF16)
            return carry
        lax.fori_loop(0, 32, zero_body, 0)

    for copy in small:
        copy.wait()
    row_scr[0], row_scr[1], lane_scr[0], lane_scr[1] = rope_angles(pos_ref[...], freq_ref[...])
    for o in (1, 2, 3):
        src = lax.rem(t + 4 - o, 4)
        for piece in range(2):
            wait_bytes(w_all.at[src, half_rows(1 - d, piece), :], wx_recv.at[src, piece])

    def emit_copy(tick, i, o, qq):
        to = lax.rem(t + o, 4)
        q = lax.rem(3 + qq, 4)
        src = xs.at[tick, i, seq_rows(to), seq_rows(q)]
        dst = emits[tick].at[8 * t + i]
        return remote(src, dst, y_send.at[tick, i], emit_recv.at[tick, o], tp=to, pp=q)

    def tick_body(tick):
        def step(i, carry):
            if tick == 0:
                x_local(i).wait()
                for o in (1, 2, 3):
                    x_arrived(i, o)
            else:
                @pl.when(p == 0)
                def _():
                    mb_local(i).wait()
                    for o in (1, 2, 3):
                        mb_arrived(i, o)

                @pl.when(p > 0)
                def _():
                    wait_bytes(xs.at[1, i], y_recv.at[i])
            layer(xs.at[tick, i], w_all, ln_scr, row_scr, lane_scr, m_scr, q_scr, k_scr, v_scr, o_scr, acc_scr)

            @pl.when(p < 3)
            def _():
                nxt = lax.min(p + 1, 3)
                if tick == 0:
                    remote(xs.at[0, i], xs.at[1, i], y_send.at[0, i], y_recv.at[i], pp=nxt).start()
                else:
                    for o in (2, 1, 3, 0):
                        to = lax.rem(t + o, 4)
                        remote(xs.at[1, i, seq_rows(to), :], final.at[0, 8 * t + i], y_send.at[1, i], final_recv.at[o],
                               tp=to, pp=nxt).start()

            @pl.when(p == 3)
            def _():
                for o in (2, 1, 3, 0):
                    for qq in (1, 2, 3, 0):
                        if o == 0 and qq == 0:
                            emits[tick][8 * t + i] = xs[tick, i, seq_rows(t), 384:512]
                        else:
                            emit_copy(tick, i, o, qq).start()
            return carry
        lax.fori_loop(0, 8, step, 0)

    tick_body(0)
    tick_body(1)

    wait_bytes(buf_ref.at[0, 0:24], xs_send)
    for _ in relay(wait_sent):
        pass

    @pl.when(p == 0)
    def _():
        wait_bytes(mb_ref.at[0:24], mb_send)

    @pl.when(p > 0)
    def _():
        for o in range(4):
            src = lax.rem(t + 4 - o, 4)
            wait_bytes(final.at[0, pl.ds(8 * src, 8)], final_recv.at[o])

    for tick in range(2):
        for o in range(4):
            @pl.when(jnp.logical_or(p < 3, o > 0))
            def _():
                wait_bytes(emits[tick].at[pl.ds(8 * lax.rem(t + 4 - o, 4), 8)], emit_recv.at[tick, o])

        def sent(i, carry):
            @pl.when(p < 3)
            def _():
                wait_bytes(xs.at[tick, i], y_send.at[tick, i])

            @pl.when(p == 3)
            def _():
                wait_bytes(emits[tick].at[0:15], y_send.at[tick, i])
            return carry
        lax.fori_loop(0, 8, sent, 0)


def solution(mesh):
    def body(stage_buf, new_mb, positions, ln_attn, ln_mlp, w_qkv, w_out, w_up, w_down):
        head_dim = w_qkv.shape[3]
        inv_freq = 1.0 / np.power(np.float32(ROPE_BASE), np.arange(0, head_dim, 2).astype(np.float32) / np.float32(head_dim))
        inv_freq = jnp.asarray(np.tile(inv_freq.astype(np.float32), 4)[None])
        batch, rows, width = new_mb.shape
        seq = 4 * rows
        emit_shape = jax.ShapeDtypeStruct((batch, rows, width // 4), BF16)
        hbm = pl.BlockSpec(memory_space=pl.ANY)
        vmem = pl.BlockSpec(memory_space=pltpu.VMEM)
        dma = pltpu.SemaphoreType.DMA
        shapes = (emit_shape, emit_shape, jax.ShapeDtypeStruct(stage_buf.shape, BF16))
        return pl.pallas_call(
            kernel,
            out_shape=tuple(pltpu.VMEM(sh.shape, BF16) for sh in shapes),
            in_specs=[hbm, hbm, vmem, vmem, hbm, hbm, hbm, hbm, hbm, hbm],
            out_specs=(vmem, vmem, vmem),
            scratch_shapes=[
                pltpu.VMEM((4, 1536, width), BF16),
                pltpu.VMEM((2, batch // 4, seq, width), BF16),
                pltpu.VMEM((2, 2, width), F32),
                pltpu.VMEM((2, seq, 128), F32),
                pltpu.VMEM((2, 64, seq), F32),
                pltpu.VMEM((seq, width), BF16),
                pltpu.VMEM((4, 128, seq), BF16),
                pltpu.VMEM((4, seq, 128), BF16),
                pltpu.VMEM((4, 128, seq), BF16),
                pltpu.VMEM((seq, width), BF16),
                pltpu.VMEM((seq, width), F32),
                dma((2, 8)), dma, dma((2,)), dma, dma((8, 3)), dma, dma((8, 3)), dma((8,)),
                dma((6, 2)), dma((4, 2)), dma((4, 2)), dma((4, 2)),
                dma((2, 8)), dma((2, 4)), dma((4,)),
            ],
            compiler_params=pltpu.CompilerParams(has_side_effects=True, collective_id=0, vmem_limit_bytes=57 * 1024 * 1024),
            cost_estimate=pl.CostEstimate(flops=60_000_000_000, bytes_accessed=40_000_000, transcendentals=50_000_000),
        )(stage_buf, new_mb, positions[None, :], inv_freq, ln_attn, ln_mlp, w_qkv, w_out, w_up, w_down)

    act_spec = P("dp", "tp", None)
    buf_spec = P("pp", "dp", "tp", None)
    emit_spec = P("dp", "tp", "pp")
    stack_spec = P("pp", None, None)
    return jax.shard_map(body, mesh=mesh, in_specs=(buf_spec, act_spec, P(None), stack_spec, stack_spec, P("pp", "tp", None, None, None), P("pp", "tp", None), P("pp", None, "tp"), P("pp", "tp", None)), out_specs=(emit_spec, emit_spec, buf_spec), check_vma=False)
```

```python
import functools

import jax
import jax.numpy as jnp
import numpy as np
from jax import lax
from jax.experimental import pallas as pl
from jax.experimental.pallas import tpu as pltpu
from jax.sharding import PartitionSpec as P

LN_EPS = 1e-5
ROPE_BASE = 10000.0
MESH = pl.DeviceIdType.MESH
NT = (((1,), (1,)), ((), ()))
F32 = jnp.float32
BF16 = jnp.bfloat16


def rope_angles(positions, inv_freq):
    seq = positions.shape[1]
    by_row = jnp.broadcast_to(positions.astype(F32), (128, seq)).T * inv_freq
    sign = jnp.where(lax.broadcasted_iota(jnp.int32, (1, 128), 1) < 64, -1.0, 1.0)
    cos_tab, sin_tab = jnp.cos(by_row), jnp.sin(by_row)
    return cos_tab, sin_tab * sign, cos_tab.T[64:128, :], sin_tab.T[64:128, :]


def layer(x_ref, w_ref, ln_ref, row_ref, lane_ref, m_scr, q_scr, k_scr, v_scr, o_scr, acc_scr):
    seq, width = x_ref.shape
    half = seq // 2

    def norm_rows(r, carry):
        rows = pl.ds(pl.multiple_of(r * half, half), half)
        x_wide = x_ref[rows, :].astype(F32)
        acc_scr[rows, :] = x_wide
        centered = x_wide - jnp.mean(x_wide, axis=-1, keepdims=True)
        variance = jnp.mean(centered * centered, axis=-1, keepdims=True)
        normed = centered * lax.rsqrt(variance + LN_EPS)
        a_norm = (normed * ln_ref[0, 0:1, :] + ln_ref[0, 1:2, :]).astype(BF16)
        m_scr[rows, :] = (normed * ln_ref[1, 0:1, :] + ln_ref[1, 1:2, :]).astype(BF16)
        w_k = w_ref[:, 256:384, :].reshape(width, width)
        keys = lax.dot_general(a_norm, w_k, NT, preferred_element_type=F32).astype(BF16).astype(F32)
        for s in range(4):
            k_wide = keys[:, 128 * s:128 * s + 128]
            k_scr[s, rows, :] = (k_wide * row_ref[0, rows, :] + pltpu.roll(k_wide, 64, 1) * row_ref[1, rows, :]).astype(BF16)
        w_qv = w_ref[:, 0:256, :].reshape(2 * width, width)
        qv = lax.dot_general(w_qv, a_norm, NT, preferred_element_type=F32).astype(BF16)
        cos_tab, sin_tab = lane_ref[0, :, rows], lane_ref[1, :, rows]
        for s in range(4):
            first, second = qv[256 * s:256 * s + 64, :].astype(F32), qv[256 * s + 64:256 * s + 128, :].astype(F32)
            q_scr[s, 0:64, rows] = (first * cos_tab - second * sin_tab).astype(BF16)
            q_scr[s, 64:128, rows] = (second * cos_tab + first * sin_tab).astype(BF16)
            v_scr[s, :, rows] = qv[256 * s + 128:256 * s + 256, :]
        return carry

    lax.fori_loop(0, 2, norm_rows, 0, unroll=2)

    def head_pair_and_mlp_part(s, carry):
        pre = jnp.dot(m_scr[...], w_ref[s, 512:1024, :], preferred_element_type=F32)
        causal = lax.broadcasted_iota(jnp.int32, (half, half), 0) <= lax.broadcasted_iota(jnp.int32, (half, half), 1)
        row = lax.broadcasted_iota(jnp.int32, (128, 1), 0)
        for hh in range(2):
            q_mask = jnp.where((row // 32) % 2 == hh, 0.125, 0.0).astype(BF16)
            for qb in range(2):
                cols = slice(qb * half, (qb + 1) * half)
                q_blk = q_scr[s, :, cols] * q_mask
                scores = [jnp.dot(k_scr[s, kb * half:(kb + 1) * half, :], q_blk, preferred_element_type=F32) for kb in range(qb + 1)]
                scores[qb] = jnp.where(causal, scores[qb], -1e30)
                peak = functools.reduce(jnp.maximum, [jnp.max(sc, axis=0, keepdims=True) for sc in scores])
                exps = [jnp.exp(sc - peak) for sc in scores]
                total = functools.reduce(jnp.add, [jnp.sum(e, axis=0, keepdims=True) for e in exps])
                probs = jnp.concatenate([e.astype(BF16) for e in exps], 0)
                head_out = jnp.dot(v_scr[s, 64 * hh:64 * hh + 64, 0:(qb + 1) * half], probs, preferred_element_type=F32)
                o_scr[pl.ds(pl.multiple_of(s * 128 + 64 * hh, 64), 64), cols] = (head_out * (1.0 / total)).astype(BF16)
        hidden = (0.5 * pre * (1.0 + lax.erf(pre * 0.7071067811865476))).astype(BF16)
        acc_scr[...] += jnp.dot(hidden, w_ref[s, 1024:1536, :], preferred_element_type=F32)
        return carry

    lax.fori_loop(0, 4, head_pair_and_mlp_part, 0, unroll=4)

    def out_rows(r, carry):
        rows = pl.ds(pl.multiple_of(r * half, half), half)
        w_out = w_ref[:, 384:512, :].reshape(width, width)
        heads = lax.dot_general(o_scr[:, rows], w_out, (((0,), (0,)), ((), ())), preferred_element_type=F32)
        x_ref[rows, :] = (acc_scr[rows, :] + heads).astype(BF16)
        return carry

    lax.fori_loop(0, 2, out_rows, 0, unroll=2)


def kernel(buf_ref, mb_ref, pos_ref, freq_ref, ln_attn, ln_mlp, w_qkv, w_out, w_up, w_down, emit_one, emit_two, final,
           w_all, xs, pos_scr, freq_scr, ln_scr, row_scr, lane_scr, m_scr, q_scr, k_scr, v_scr, o_scr, acc_scr,
           loc_sem, wloc_sem, ln_sem, xs_send, xs_recv, mb_send, mb_recv, y_recv, wz_send, wz_recv, wx_send, wx_recv,
           y_send, emit_recv, final_recv):
    d, t, p = lax.axis_index("dp"), lax.axis_index("tp"), lax.axis_index("pp")
    emits = (emit_one, emit_two)

    def remote(src, dst, send, recv, dp=None, tp=None, pp=None):
        where = (d if dp is None else dp, t if tp is None else tp, p if pp is None else pp)
        return pltpu.make_async_remote_copy(src, dst, send, recv, device_id=where, device_id_type=MESH)

    def wait_bytes(ref, sem):
        pltpu.make_async_copy(ref, ref, sem).wait()

    def seq_rows(rank):
        return pl.ds(pl.multiple_of(rank * 128, 128), 128)

    def x_copy(i, o):
        to = lax.rem(t + o, 4)
        return remote(buf_ref.at[0, 8 * to + i], xs.at[0, i, seq_rows(t), :], xs_send, xs_recv.at[i, o - 1], tp=to)

    def x_arrived(i, o):
        src = lax.rem(t + 4 - o, 4)
        wait_bytes(xs.at[0, i, seq_rows(src), :], xs_recv.at[i, o - 1])

    def mb_copy(i, o):
        to = lax.rem(t + o, 4)
        return remote(mb_ref.at[8 * to + i], xs.at[1, i, seq_rows(t), :], mb_send, mb_recv.at[i, o - 1], tp=to)

    def mb_arrived(i, o):
        src = lax.rem(t + 4 - o, 4)
        wait_bytes(xs.at[1, i, seq_rows(src), :], mb_recv.at[i, o - 1])

    def x_local(i):
        return pltpu.make_async_copy(buf_ref.at[0, 8 * t + i], xs.at[0, i, seq_rows(t), :], loc_sem.at[0, i])

    def mb_local(i):
        return pltpu.make_async_copy(mb_ref.at[8 * t + i], xs.at[1, i, seq_rows(t), :], loc_sem.at[1, i])

    def send_x(i):
        for o in (2, 1, 3):
            x_copy(i, o).start()

    def half_rows(dp, piece):
        size = 256 * (piece + 1)
        return pl.ds(pl.multiple_of(512 * piece + dp * size, 256), size)

    def w_copy_z(s, piece, to, slot):
        rows = half_rows(d, piece)
        return remote(w_all.at[s, rows, :], w_all.at[s, rows, :], wz_send.at[slot, piece], wz_recv.at[s, piece], tp=to)

    def w_copy_x(s, piece):
        rows = half_rows(d, piece)
        return remote(w_all.at[s, rows, :], w_all.at[s, rows, :], wx_send.at[s, piece], wx_recv.at[s, piece], dp=1 - d)

    def relay(action):
        for hop in range(4):
            for piece in range(2):
                right_src, left_src = lax.max(t - hop, 0), lax.min(t + hop, 3)
                from_left, from_right = t >= hop, t + hop <= 3
                if hop:
                    for arrived, s in ((from_left, right_src), (from_right, left_src)):
                        @pl.when(arrived)
                        def _():
                            action("arrive", None, s, piece)
                if hop < 3:
                    @pl.when(jnp.logical_and(from_left, t < 3))
                    def _():
                        action("z", w_copy_z(right_src, piece, lax.min(t + 1, 3), 2 * hop), right_src, piece)

                    @pl.when(jnp.logical_and(from_right, t > 0))
                    def _():
                        action("z", w_copy_z(left_src, piece, lax.max(t - 1, 0), 2 * hop + 1), left_src, piece)
                if hop:
                    for arrived, s in ((from_left, right_src), (from_right, left_src)):
                        @pl.when(arrived)
                        def _():
                            action("x", w_copy_x(s, piece), s, piece)
            yield hop

    def start_or_wait(kind, copy, s, piece):
        if kind == "arrive":
            wait_bytes(w_all.at[s, half_rows(d, piece), :], wz_recv.at[s, piece])
        else:
            copy.start()

    def wait_sent(kind, copy, s, piece):
        if kind != "arrive":
            copy.wait_send()

    barrier = pltpu.get_barrier_semaphore()
    for o in range(4):
        for oo in range(4):
            if o or oo:
                where = (d, lax.rem(t + o, 4), lax.rem(p + oo, 4))
                pl.semaphore_signal(barrier, inc=1, device_id=where, device_id_type=MESH)
    pl.semaphore_signal(barrier, inc=1, device_id=(1 - d, t, p), device_id_type=MESH)

    own = []
    for head in range(2):
        for j, row in ((0, 0), (1, 256)):
            for side in range(2):
                own.append((w_qkv.at[0, head, j, pl.ds(32 * side, 32), :], row + 64 * side + 32 * head, 32))
        own.append((w_qkv.at[0, head, 2], 128 + 64 * head, 64))
    own += [(w_out.at[0], 384, 128), (w_up.at[0], 512, 512), (w_down.at[0], 1024, 512)]
    for src, row, size in own:
        pltpu.make_async_copy(src, w_all.at[t, pl.ds(row, size), :], wloc_sem).start()
    small = [pltpu.make_async_copy(ln_attn.at[0], ln_scr.at[0], ln_sem.at[0]), pltpu.make_async_copy(ln_mlp.at[0], ln_scr.at[1], ln_sem.at[1]),
             pltpu.make_async_copy(pos_ref, pos_scr, ln_sem.at[2]), pltpu.make_async_copy(freq_ref, freq_scr, ln_sem.at[3])]
    for copy in small:
        copy.start()
    for i in range(8):
        x_local(i).start()

    pl.semaphore_wait(barrier, 16)

    send_x(0)
    wait_bytes(w_all.at[t], wloc_sem)
    for hop in relay(start_or_wait):
        for i in ((), (1, 2), (3, 4), (5, 6, 7))[hop]:
            send_x(i)

    @pl.when(p == 0)
    def _():
        def body(i, carry):
            mb_local(i).start()
            for o in (2, 1, 3):
                mb_copy(i, o).start()
            return carry
        lax.fori_loop(0, 8, body, 0)

        def zero_body(i, carry):
            final[0, i] = jnp.zeros(final.shape[2:], BF16)
            return carry
        lax.fori_loop(0, 32, zero_body, 0)

    for copy in small:
        copy.wait()
    row_scr[0], row_scr[1], lane_scr[0], lane_scr[1] = rope_angles(pos_scr[...], freq_scr[...])
    for o in (1, 2, 3):
        src = lax.rem(t + 4 - o, 4)
        for piece in range(2):
            wait_bytes(w_all.at[src, half_rows(1 - d, piece), :], wx_recv.at[src, piece])

    def emit_copy(tick, i, o, qq):
        to = lax.rem(t + o, 4)
        q = lax.rem(3 + qq, 4)
        src = xs.at[tick, i, seq_rows(to), seq_rows(q)]
        dst = emits[tick].at[8 * t + i]
        return remote(src, dst, y_send.at[tick, i], emit_recv.at[tick, o], tp=to, pp=q)

    def tick_body(tick):
        def step(i, carry):
            if tick == 0:
                x_local(i).wait()
                for o in (1, 2, 3):
                    x_arrived(i, o)
            else:
                @pl.when(p == 0)
                def _():
                    mb_local(i).wait()
                    for o in (1, 2, 3):
                        mb_arrived(i, o)

                @pl.when(p > 0)
                def _():
                    wait_bytes(xs.at[1, i], y_recv.at[i])
            layer(xs.at[tick, i], w_all, ln_scr, row_scr, lane_scr, m_scr, q_scr, k_scr, v_scr, o_scr, acc_scr)

            @pl.when(p < 3)
            def _():
                nxt = lax.min(p + 1, 3)
                if tick == 0:
                    remote(xs.at[0, i], xs.at[1, i], y_send.at[0, i], y_recv.at[i], pp=nxt).start()
                else:
                    for o in (2, 1, 3, 0):
                        to = lax.rem(t + o, 4)
                        remote(xs.at[1, i, seq_rows(to), :], final.at[0, 8 * t + i], y_send.at[1, i], final_recv.at[o],
                               tp=to, pp=nxt).start()

            @pl.when(p == 3)
            def _():
                for o in (2, 1, 3, 0):
                    for qq in (1, 2, 3, 0):
                        if o == 0 and qq == 0:
                            emits[tick][8 * t + i] = xs[tick, i, seq_rows(t), 384:512]
                        else:
                            emit_copy(tick, i, o, qq).start()
            return carry
        lax.fori_loop(0, 8, step, 0)

    tick_body(0)
    tick_body(1)

    wait_bytes(buf_ref.at[0, 0:24], xs_send)
    for _ in relay(wait_sent):
        pass

    @pl.when(p == 0)
    def _():
        wait_bytes(mb_ref.at[0:24], mb_send)

    @pl.when(p > 0)
    def _():
        for o in range(4):
            src = lax.rem(t + 4 - o, 4)
            wait_bytes(final.at[0, pl.ds(8 * src, 8)], final_recv.at[o])

    for tick in range(2):
        for o in range(4):
            @pl.when(jnp.logical_or(p < 3, o > 0))
            def _():
                wait_bytes(emits[tick].at[pl.ds(8 * lax.rem(t + 4 - o, 4), 8)], emit_recv.at[tick, o])

        def sent(i, carry):
            @pl.when(p < 3)
            def _():
                wait_bytes(xs.at[tick, i], y_send.at[tick, i])

            @pl.when(p == 3)
            def _():
                wait_bytes(emits[tick].at[0:15], y_send.at[tick, i])
            return carry
        lax.fori_loop(0, 8, sent, 0)


def unload(*refs):
    copies = []
    for j in range(3):
        source, target = (refs[j].at[0], refs[3 + j].at[0]) if j == 2 else (refs[j], refs[3 + j])
        step = source.shape[0] // (4 if j == 2 else 1)
        for k in range(0, source.shape[0], step):
            copies.append(pltpu.make_async_copy(source.at[pl.ds(k, step)], target.at[pl.ds(k, step)], refs[6].at[len(copies)]))
    for copy in copies:
        copy.start()
    for copy in copies:
        copy.wait()


def solution(mesh):
    def body(stage_buf, new_mb, positions, ln_attn, ln_mlp, w_qkv, w_out, w_up, w_down):
        head_dim = w_qkv.shape[3]
        inv_freq = 1.0 / np.power(np.float32(ROPE_BASE), np.arange(0, head_dim, 2).astype(np.float32) / np.float32(head_dim))
        inv_freq = jnp.asarray(np.tile(inv_freq.astype(np.float32), 4)[None])
        batch, rows, width = new_mb.shape
        seq = 4 * rows
        emit_shape = jax.ShapeDtypeStruct((batch, rows, width // 4), BF16)
        hbm = pl.BlockSpec(memory_space=pl.ANY)
        vmem = pl.BlockSpec(memory_space=pltpu.VMEM)
        dma = pltpu.SemaphoreType.DMA
        shapes = (emit_shape, emit_shape, jax.ShapeDtypeStruct(stage_buf.shape, BF16))
        landed = pl.pallas_call(
            kernel,
            out_shape=tuple(pltpu.VMEM(sh.shape, BF16) for sh in shapes),
            in_specs=[hbm, hbm, hbm, hbm, hbm, hbm, hbm, hbm, hbm, hbm],
            out_specs=(vmem, vmem, vmem),
            scratch_shapes=[
                pltpu.VMEM((4, 1536, width), BF16),
                pltpu.VMEM((2, batch // 4, seq, width), BF16),
                pltpu.VMEM((1, seq), jnp.int32),
                pltpu.VMEM((1, 128), F32),
                pltpu.VMEM((2, 2, width), F32),
                pltpu.VMEM((2, seq, 128), F32),
                pltpu.VMEM((2, 64, seq), F32),
                pltpu.VMEM((seq, width), BF16),
                pltpu.VMEM((4, 128, seq), BF16),
                pltpu.VMEM((4, seq, 128), BF16),
                pltpu.VMEM((4, 128, seq), BF16),
                pltpu.VMEM((seq, width), BF16),
                pltpu.VMEM((seq, width), F32),
                dma((2, 8)), dma, dma((4,)), dma, dma((8, 3)), dma, dma((8, 3)), dma((8,)),
                dma((6, 2)), dma((4, 2)), dma((4, 2)), dma((4, 2)),
                dma((2, 8)), dma((2, 4)), dma((4,)),
            ],
            compiler_params=pltpu.CompilerParams(has_side_effects=True, collective_id=0, vmem_limit_bytes=57 * 1024 * 1024),
            cost_estimate=pl.CostEstimate(flops=60_000_000_000, bytes_accessed=40_000_000, transcendentals=50_000_000),
        )(stage_buf, new_mb, positions[None, :], inv_freq, ln_attn, ln_mlp, w_qkv, w_out, w_up, w_down)
        landed = [pltpu.with_memory_space_constraint(x, pltpu.VMEM) for x in landed]
        return pl.pallas_call(
            unload,
            out_shape=shapes,
            in_specs=[vmem, vmem, vmem],
            out_specs=(hbm, hbm, hbm),
            scratch_shapes=[dma((6,))],
            compiler_params=pltpu.CompilerParams(vmem_limit_bytes=1024 * 1024),
            cost_estimate=pl.CostEstimate(flops=1_000_000, bytes_accessed=12_000_000, transcendentals=0),
        )(*landed)

    act_spec = P("dp", "tp", None)
    buf_spec = P("pp", "dp", "tp", None)
    emit_spec = P("dp", "tp", "pp")
    stack_spec = P("pp", None, None)
    return jax.shard_map(body, mesh=mesh, in_specs=(buf_spec, act_spec, P(None), stack_spec, stack_spec, P("pp", "tp", None, None, None), P("pp", "tp", None), P("pp", None, "tp"), P("pp", "tp", None)), out_specs=(emit_spec, emit_spec, buf_spec), check_vma=False)
```

```python
import functools

import jax
import jax.numpy as jnp
import numpy as np
from jax import lax
from jax.experimental import pallas as pl
from jax.experimental.pallas import tpu as pltpu
from jax.sharding import PartitionSpec as P

LN_EPS = 1e-5
ROPE_BASE = 10000.0
MESH = pl.DeviceIdType.MESH
NT = (((1,), (1,)), ((), ()))
F32 = jnp.float32
BF16 = jnp.bfloat16


def rope_angles(positions, inv_freq):
    seq = positions.shape[1]
    by_row = jnp.broadcast_to(positions.astype(F32), (128, seq)).T * inv_freq
    sign = jnp.where(lax.broadcasted_iota(jnp.int32, (1, 128), 1) < 64, -1.0, 1.0)
    cos_tab, sin_tab = jnp.cos(by_row), jnp.sin(by_row)
    return cos_tab, sin_tab * sign, cos_tab.T[64:128, :], sin_tab.T[64:128, :]


def layer(x_ref, w_ref, ln_ref, row_ref, lane_ref, m_scr, q_scr, k_scr, v_scr, o_scr, acc_scr):
    seq, width = x_ref.shape
    half = seq // 2

    def norm_rows(r, carry):
        rows = pl.ds(pl.multiple_of(r * half, half), half)
        x_wide = x_ref[rows, :].astype(F32)
        acc_scr[rows, :] = x_wide
        centered = x_wide - jnp.mean(x_wide, axis=-1, keepdims=True)
        variance = jnp.mean(centered * centered, axis=-1, keepdims=True)
        normed = centered * lax.rsqrt(variance + LN_EPS)
        a_norm = (normed * ln_ref[0, 0:1, :] + ln_ref[0, 1:2, :]).astype(BF16)
        m_scr[rows, :] = (normed * ln_ref[1, 0:1, :] + ln_ref[1, 1:2, :]).astype(BF16)
        w_k = w_ref[:, 256:384, :].reshape(width, width)
        keys = lax.dot_general(a_norm, w_k, NT, preferred_element_type=F32).astype(BF16).astype(F32)
        for s in range(4):
            k_wide = keys[:, 128 * s:128 * s + 128]
            k_scr[s, rows, :] = (k_wide * row_ref[0, rows, :] + pltpu.roll(k_wide, 64, 1) * row_ref[1, rows, :]).astype(BF16)
        w_qv = w_ref[:, 0:256, :].reshape(2 * width, width)
        qv = lax.dot_general(w_qv, a_norm, NT, preferred_element_type=F32).astype(BF16)
        cos_tab, sin_tab = lane_ref[0, :, rows], lane_ref[1, :, rows]
        for s in range(4):
            first, second = qv[256 * s:256 * s + 64, :].astype(F32), qv[256 * s + 64:256 * s + 128, :].astype(F32)
            q_scr[s, 0:64, rows] = (first * cos_tab - second * sin_tab).astype(BF16)
            q_scr[s, 64:128, rows] = (second * cos_tab + first * sin_tab).astype(BF16)
            v_scr[s, :, rows] = qv[256 * s + 128:256 * s + 256, :]
        return carry

    lax.fori_loop(0, 2, norm_rows, 0, unroll=2)

    def head_pair_and_mlp_part(s, carry):
        pre = jnp.dot(m_scr[...], w_ref[s, 512:1024, :], preferred_element_type=F32)
        causal = lax.broadcasted_iota(jnp.int32, (half, half), 0) <= lax.broadcasted_iota(jnp.int32, (half, half), 1)
        row = lax.broadcasted_iota(jnp.int32, (128, 1), 0)
        for hh in range(2):
            q_mask = jnp.where((row // 32) % 2 == hh, 0.125, 0.0).astype(BF16)
            for qb in range(2):
                cols = slice(qb * half, (qb + 1) * half)
                q_blk = q_scr[s, :, cols] * q_mask
                scores = [jnp.dot(k_scr[s, kb * half:(kb + 1) * half, :], q_blk, preferred_element_type=F32) for kb in range(qb + 1)]
                scores[qb] = jnp.where(causal, scores[qb], -1e30)
                peak = functools.reduce(jnp.maximum, [jnp.max(sc, axis=0, keepdims=True) for sc in scores])
                exps = [jnp.exp(sc - peak) for sc in scores]
                total = functools.reduce(jnp.add, [jnp.sum(e, axis=0, keepdims=True) for e in exps])
                probs = jnp.concatenate([e.astype(BF16) for e in exps], 0)
                head_out = jnp.dot(v_scr[s, 64 * hh:64 * hh + 64, 0:(qb + 1) * half], probs, preferred_element_type=F32)
                o_scr[pl.ds(pl.multiple_of(s * 128 + 64 * hh, 64), 64), cols] = (head_out * (1.0 / total)).astype(BF16)
        hidden = (0.5 * pre * (1.0 + lax.erf(pre * 0.7071067811865476))).astype(BF16)
        acc_scr[...] += jnp.dot(hidden, w_ref[s, 1024:1536, :], preferred_element_type=F32)
        return carry

    lax.fori_loop(0, 4, head_pair_and_mlp_part, 0, unroll=4)

    def out_rows(r, carry):
        rows = pl.ds(pl.multiple_of(r * half, half), half)
        w_out = w_ref[:, 384:512, :].reshape(width, width)
        heads = lax.dot_general(o_scr[:, rows], w_out, (((0,), (0,)), ((), ())), preferred_element_type=F32)
        x_ref[rows, :] = (acc_scr[rows, :] + heads).astype(BF16)
        return carry

    lax.fori_loop(0, 2, out_rows, 0, unroll=2)


def kernel(buf_ref, mb_ref, pos_ref, freq_ref, ln_attn, ln_mlp, w_qkv, w_out, w_up, w_down, emit_one, emit_two, final,
           w_all, xs, pos_scr, freq_scr, ln_scr, row_scr, lane_scr, m_scr, q_scr, k_scr, v_scr, o_scr, acc_scr,
           loc_sem, wloc_sem, ln_sem, xs_send, xs_recv, mb_send, mb_recv, y_recv, wz_send, wz_recv, wx_send, wx_recv,
           y_send, emit_recv, final_recv, column_sem):
    d, t, p = lax.axis_index("dp"), lax.axis_index("tp"), lax.axis_index("pp")
    emits = (emit_one, emit_two)

    def remote(src, dst, send, recv, dp=None, tp=None, pp=None):
        where = (d if dp is None else dp, t if tp is None else tp, p if pp is None else pp)
        return pltpu.make_async_remote_copy(src, dst, send, recv, device_id=where, device_id_type=MESH)

    def wait_bytes(ref, sem):
        pltpu.make_async_copy(ref, ref, sem).wait()

    def seq_rows(rank):
        return pl.ds(pl.multiple_of(rank * 128, 128), 128)

    def x_copy(i, o):
        to = lax.rem(t + o, 4)
        return remote(buf_ref.at[0, 8 * to + i], xs.at[0, i, seq_rows(t), :], xs_send, xs_recv.at[i, o - 1], tp=to)

    def x_arrived(i, o):
        src = lax.rem(t + 4 - o, 4)
        wait_bytes(xs.at[0, i, seq_rows(src), :], xs_recv.at[i, o - 1])

    def mb_copy(i, o):
        to = lax.rem(t + o, 4)
        return remote(mb_ref.at[8 * to + i], xs.at[1, i, seq_rows(t), :], mb_send, mb_recv.at[i, o - 1], tp=to)

    def mb_arrived(i, o):
        src = lax.rem(t + 4 - o, 4)
        wait_bytes(xs.at[1, i, seq_rows(src), :], mb_recv.at[i, o - 1])

    def x_local(i):
        return pltpu.make_async_copy(buf_ref.at[0, 8 * t + i], xs.at[0, i, seq_rows(t), :], loc_sem.at[0, i])

    def mb_local(i):
        return pltpu.make_async_copy(mb_ref.at[8 * t + i], xs.at[1, i, seq_rows(t), :], loc_sem.at[1, i])

    def send_x(i):
        for o in (2, 1, 3):
            x_copy(i, o).start()

    def half_rows(dp, piece):
        size = 256 * (piece + 1)
        return pl.ds(pl.multiple_of(512 * piece + dp * size, 256), size)

    def w_copy_z(s, piece, to, slot):
        rows = half_rows(d, piece)
        return remote(w_all.at[s, rows, :], w_all.at[s, rows, :], wz_send.at[slot, piece], wz_recv.at[s, piece], tp=to)

    def w_copy_x(s, piece):
        rows = half_rows(d, piece)
        return remote(w_all.at[s, rows, :], w_all.at[s, rows, :], wx_send.at[s, piece], wx_recv.at[s, piece], dp=1 - d)

    def relay(action):
        for hop in range(4):
            for piece in range(2):
                right_src, left_src = lax.max(t - hop, 0), lax.min(t + hop, 3)
                from_left, from_right = t >= hop, t + hop <= 3
                if hop:
                    for arrived, s in ((from_left, right_src), (from_right, left_src)):
                        @pl.when(arrived)
                        def _():
                            action("arrive", None, s, piece)
                if hop < 3:
                    @pl.when(jnp.logical_and(from_left, t < 3))
                    def _():
                        action("z", w_copy_z(right_src, piece, lax.min(t + 1, 3), 2 * hop), right_src, piece)

                    @pl.when(jnp.logical_and(from_right, t > 0))
                    def _():
                        action("z", w_copy_z(left_src, piece, lax.max(t - 1, 0), 2 * hop + 1), left_src, piece)
                if hop:
                    for arrived, s in ((from_left, right_src), (from_right, left_src)):
                        @pl.when(arrived)
                        def _():
                            action("x", w_copy_x(s, piece), s, piece)
            yield hop

    def start_or_wait(kind, copy, s, piece):
        if kind == "arrive":
            wait_bytes(w_all.at[s, half_rows(d, piece), :], wz_recv.at[s, piece])
        else:
            copy.start()

    def wait_sent(kind, copy, s, piece):
        if kind != "arrive":
            copy.wait_send()

    barrier = pltpu.get_barrier_semaphore()
    for o in (1, 2, 3):
        pl.semaphore_signal(barrier, inc=1, device_id=(d, lax.rem(t + o, 4), p), device_id_type=MESH)
        pl.semaphore_signal(barrier, inc=1, device_id=(d, t, lax.rem(p + o, 4)), device_id_type=MESH)
    pl.semaphore_signal(barrier, inc=1, device_id=(1 - d, t, p), device_id_type=MESH)

    own = []
    for head in range(2):
        for j, row in ((0, 0), (1, 256)):
            for side in range(2):
                own.append((w_qkv.at[0, head, j, pl.ds(32 * side, 32), :], row + 64 * side + 32 * head, 32))
        own.append((w_qkv.at[0, head, 2], 128 + 64 * head, 64))
    own += [(w_out.at[0], 384, 128), (w_up.at[0], 512, 512), (w_down.at[0], 1024, 512)]
    for src, row, size in own:
        pltpu.make_async_copy(src, w_all.at[t, pl.ds(row, size), :], wloc_sem).start()
    small = [pltpu.make_async_copy(ln_attn.at[0], ln_scr.at[0], ln_sem.at[0]), pltpu.make_async_copy(ln_mlp.at[0], ln_scr.at[1], ln_sem.at[1]),
             pltpu.make_async_copy(pos_ref, pos_scr, ln_sem.at[2]), pltpu.make_async_copy(freq_ref, freq_scr, ln_sem.at[3])]
    for copy in small:
        copy.start()
    for i in range(8):
        x_local(i).start()

    pl.semaphore_wait(barrier, 7)

    send_x(0)
    for o in (1, 2, 3):
        pl.semaphore_signal(column_sem, inc=1, device_id=(d, lax.rem(t + o, 4), p), device_id_type=MESH)
    wait_bytes(w_all.at[t], wloc_sem)
    for hop in relay(start_or_wait):
        for i in ((), (1, 2), (3, 4), (5, 6, 7))[hop]:
            send_x(i)

    @pl.when(p == 0)
    def _():
        def body(i, carry):
            mb_local(i).start()
            for o in (2, 1, 3):
                mb_copy(i, o).start()
            return carry
        lax.fori_loop(0, 8, body, 0)

        def zero_body(i, carry):
            final[0, i] = jnp.zeros(final.shape[2:], BF16)
            return carry
        lax.fori_loop(0, 32, zero_body, 0)

    for copy in small:
        copy.wait()
    row_scr[0], row_scr[1], lane_scr[0], lane_scr[1] = rope_angles(pos_scr[...], freq_scr[...])
    for o in (1, 2, 3):
        src = lax.rem(t + 4 - o, 4)
        for piece in range(2):
            wait_bytes(w_all.at[src, half_rows(1 - d, piece), :], wx_recv.at[src, piece])

    def emit_copy(tick, i, o, qq):
        to = lax.rem(t + o, 4)
        q = lax.rem(3 + qq, 4)
        src = xs.at[tick, i, seq_rows(to), seq_rows(q)]
        dst = emits[tick].at[8 * t + i]
        return remote(src, dst, y_send.at[tick, i], emit_recv.at[tick, o], tp=to, pp=q)

    def tick_body(tick):
        def step(i, carry):
            if tick == 0:
                x_local(i).wait()
                for o in (1, 2, 3):
                    x_arrived(i, o)
            else:
                @pl.when(p == 0)
                def _():
                    mb_local(i).wait()
                    for o in (1, 2, 3):
                        mb_arrived(i, o)

                @pl.when(p > 0)
                def _():
                    wait_bytes(xs.at[1, i], y_recv.at[i])
            layer(xs.at[tick, i], w_all, ln_scr, row_scr, lane_scr, m_scr, q_scr, k_scr, v_scr, o_scr, acc_scr)

            @pl.when(p < 3)
            def _():
                nxt = lax.min(p + 1, 3)
                if tick == 0:
                    remote(xs.at[0, i], xs.at[1, i], y_send.at[0, i], y_recv.at[i], pp=nxt).start()
                else:
                    for o in (2, 1, 3, 0):
                        to = lax.rem(t + o, 4)
                        remote(xs.at[1, i, seq_rows(to), :], final.at[0, 8 * t + i], y_send.at[1, i], final_recv.at[o],
                               tp=to, pp=nxt).start()

            @pl.when(p == 3)
            def _():
                for o in (2, 1, 3, 0):
                    for qq in (1, 2, 3, 0):
                        if o == 0 and qq == 0:
                            emits[tick][8 * t + i] = xs[tick, i, seq_rows(t), 384:512]
                        else:
                            emit_copy(tick, i, o, qq).start()
            return carry
        lax.fori_loop(0, 8, step, 0)

    pl.semaphore_wait(column_sem, 3)
    tick_body(0)
    tick_body(1)

    wait_bytes(buf_ref.at[0, 0:24], xs_send)
    for _ in relay(wait_sent):
        pass

    @pl.when(p == 0)
    def _():
        wait_bytes(mb_ref.at[0:24], mb_send)

    @pl.when(p > 0)
    def _():
        for o in range(4):
            src = lax.rem(t + 4 - o, 4)
            wait_bytes(final.at[0, pl.ds(8 * src, 8)], final_recv.at[o])

    for tick in range(2):
        for o in range(4):
            @pl.when(jnp.logical_or(p < 3, o > 0))
            def _():
                wait_bytes(emits[tick].at[pl.ds(8 * lax.rem(t + 4 - o, 4), 8)], emit_recv.at[tick, o])

        def sent(i, carry):
            @pl.when(p < 3)
            def _():
                wait_bytes(xs.at[tick, i], y_send.at[tick, i])

            @pl.when(p == 3)
            def _():
                wait_bytes(emits[tick].at[0:15], y_send.at[tick, i])
            return carry
        lax.fori_loop(0, 8, sent, 0)


def unload(*refs):
    copies = []
    for j in range(3):
        source, target = (refs[j].at[0], refs[3 + j].at[0]) if j == 2 else (refs[j], refs[3 + j])
        step = source.shape[0] // (4 if j == 2 else 1)
        for k in range(0, source.shape[0], step):
            copies.append(pltpu.make_async_copy(source.at[pl.ds(k, step)], target.at[pl.ds(k, step)], refs[6].at[len(copies)]))
    for copy in copies:
        copy.start()
    for copy in copies:
        copy.wait()


def solution(mesh):
    def body(stage_buf, new_mb, positions, ln_attn, ln_mlp, w_qkv, w_out, w_up, w_down):
        head_dim = w_qkv.shape[3]
        inv_freq = 1.0 / np.power(np.float32(ROPE_BASE), np.arange(0, head_dim, 2).astype(np.float32) / np.float32(head_dim))
        inv_freq = jnp.asarray(np.tile(inv_freq.astype(np.float32), 4)[None])
        batch, rows, width = new_mb.shape
        seq = 4 * rows
        emit_shape = jax.ShapeDtypeStruct((batch, rows, width // 4), BF16)
        hbm = pl.BlockSpec(memory_space=pl.ANY)
        vmem = pl.BlockSpec(memory_space=pltpu.VMEM)
        dma = pltpu.SemaphoreType.DMA
        shapes = (emit_shape, emit_shape, jax.ShapeDtypeStruct(stage_buf.shape, BF16))
        landed = pl.pallas_call(
            kernel,
            out_shape=tuple(pltpu.VMEM(sh.shape, BF16) for sh in shapes),
            in_specs=[hbm, hbm, hbm, hbm, hbm, hbm, hbm, hbm, hbm, hbm],
            out_specs=(vmem, vmem, vmem),
            scratch_shapes=[
                pltpu.VMEM((4, 1536, width), BF16),
                pltpu.VMEM((2, batch // 4, seq, width), BF16),
                pltpu.VMEM((1, seq), jnp.int32),
                pltpu.VMEM((1, 128), F32),
                pltpu.VMEM((2, 2, width), F32),
                pltpu.VMEM((2, seq, 128), F32),
                pltpu.VMEM((2, 64, seq), F32),
                pltpu.VMEM((seq, width), BF16),
                pltpu.VMEM((4, 128, seq), BF16),
                pltpu.VMEM((4, seq, 128), BF16),
                pltpu.VMEM((4, 128, seq), BF16),
                pltpu.VMEM((seq, width), BF16),
                pltpu.VMEM((seq, width), F32),
                dma((2, 8)), dma, dma((4,)), dma, dma((8, 3)), dma, dma((8, 3)), dma((8,)),
                dma((6, 2)), dma((4, 2)), dma((4, 2)), dma((4, 2)),
                dma((2, 8)), dma((2, 4)), dma((4,)), pltpu.SemaphoreType.REGULAR,
            ],
            compiler_params=pltpu.CompilerParams(has_side_effects=True, collective_id=0, vmem_limit_bytes=57 * 1024 * 1024),
            cost_estimate=pl.CostEstimate(flops=60_000_000_000, bytes_accessed=40_000_000, transcendentals=50_000_000),
        )(stage_buf, new_mb, positions[None, :], inv_freq, ln_attn, ln_mlp, w_qkv, w_out, w_up, w_down)
        landed = [pltpu.with_memory_space_constraint(x, pltpu.VMEM) for x in landed]
        return pl.pallas_call(
            unload,
            out_shape=shapes,
            in_specs=[vmem, vmem, vmem],
            out_specs=(hbm, hbm, hbm),
            scratch_shapes=[dma((6,))],
            compiler_params=pltpu.CompilerParams(vmem_limit_bytes=1024 * 1024),
            cost_estimate=pl.CostEstimate(flops=1_000_000, bytes_accessed=12_000_000, transcendentals=0),
        )(*landed)

    act_spec = P("dp", "tp", None)
    buf_spec = P("pp", "dp", "tp", None)
    emit_spec = P("dp", "tp", "pp")
    stack_spec = P("pp", None, None)
    return jax.shard_map(body, mesh=mesh, in_specs=(buf_spec, act_spec, P(None), stack_spec, stack_spec, P("pp", "tp", None, None, None), P("pp", "tp", None), P("pp", None, "tp"), P("pp", "tp", None)), out_specs=(emit_spec, emit_spec, buf_spec), check_vma=False)
```

```python
import functools

import jax
import jax.numpy as jnp
import numpy as np
from jax import lax
from jax.experimental import pallas as pl
from jax.experimental.pallas import tpu as pltpu
from jax.sharding import PartitionSpec as P

LN_EPS = 1e-5
ROPE_BASE = 10000.0
MESH = pl.DeviceIdType.MESH
NT = (((1,), (1,)), ((), ()))
F32 = jnp.float32
BF16 = jnp.bfloat16


def rope_angles(positions, inv_freq):
    seq = positions.shape[1]
    by_row = jnp.broadcast_to(positions.astype(F32), (128, seq)).T * inv_freq
    sign = jnp.where(lax.broadcasted_iota(jnp.int32, (1, 128), 1) < 64, -1.0, 1.0)
    cos_tab, sin_tab = jnp.cos(by_row), jnp.sin(by_row)
    return cos_tab, sin_tab * sign, cos_tab.T[64:128, :], sin_tab.T[64:128, :]


def layer(x_ref, w_ref, ln_ref, row_ref, lane_ref, m_scr, q_scr, k_scr, v_scr, o_scr, acc_scr):
    seq, width = x_ref.shape
    half = seq // 2

    def norm_rows(r, carry):
        rows = pl.ds(pl.multiple_of(r * half, half), half)
        x_wide = x_ref[rows, :].astype(F32)
        acc_scr[rows, :] = x_wide
        centered = x_wide - jnp.mean(x_wide, axis=-1, keepdims=True)
        variance = jnp.mean(centered * centered, axis=-1, keepdims=True)
        normed = centered * lax.rsqrt(variance + LN_EPS)
        a_norm = (normed * ln_ref[0, 0:1, :] + ln_ref[0, 1:2, :]).astype(BF16)
        m_scr[rows, :] = (normed * ln_ref[1, 0:1, :] + ln_ref[1, 1:2, :]).astype(BF16)
        w_k = w_ref[:, 256:384, :].reshape(width, width)
        keys = lax.dot_general(a_norm, w_k, NT, preferred_element_type=F32).astype(BF16).astype(F32)
        for s in range(4):
            k_wide = keys[:, 128 * s:128 * s + 128]
            k_scr[s, rows, :] = (k_wide * row_ref[0, rows, :] + pltpu.roll(k_wide, 64, 1) * row_ref[1, rows, :]).astype(BF16)
        w_qv = w_ref[:, 0:256, :].reshape(2 * width, width)
        qv = lax.dot_general(w_qv, a_norm, NT, preferred_element_type=F32).astype(BF16)
        cos_tab, sin_tab = lane_ref[0, :, rows], lane_ref[1, :, rows]
        for s in range(4):
            first, second = qv[256 * s:256 * s + 64, :].astype(F32), qv[256 * s + 64:256 * s + 128, :].astype(F32)
            q_scr[s, 0:64, rows] = (first * cos_tab - second * sin_tab).astype(BF16)
            q_scr[s, 64:128, rows] = (second * cos_tab + first * sin_tab).astype(BF16)
            v_scr[s, :, rows] = qv[256 * s + 128:256 * s + 256, :]
        return carry

    lax.fori_loop(0, 2, norm_rows, 0, unroll=2)

    def head_pair_and_mlp_part(s, carry):
        pre = jnp.dot(m_scr[...], w_ref[s, 512:1024, :], preferred_element_type=F32)
        causal = lax.broadcasted_iota(jnp.int32, (half, half), 0) <= lax.broadcasted_iota(jnp.int32, (half, half), 1)
        row = lax.broadcasted_iota(jnp.int32, (128, 1), 0)
        for hh in range(2):
            q_mask = jnp.where((row // 32) % 2 == hh, 0.125, 0.0).astype(BF16)
            for qb in range(2):
                cols = slice(qb * half, (qb + 1) * half)
                q_blk = q_scr[s, :, cols] * q_mask
                scores = [jnp.dot(k_scr[s, kb * half:(kb + 1) * half, :], q_blk, preferred_element_type=F32) for kb in range(qb + 1)]
                scores[qb] = jnp.where(causal, scores[qb], -1e30)
                peak = functools.reduce(jnp.maximum, [jnp.max(sc, axis=0, keepdims=True) for sc in scores])
                exps = [jnp.exp(sc - peak) for sc in scores]
                total = functools.reduce(jnp.add, [jnp.sum(e, axis=0, keepdims=True) for e in exps])
                probs = jnp.concatenate([e.astype(BF16) for e in exps], 0)
                head_out = jnp.dot(v_scr[s, 64 * hh:64 * hh + 64, 0:(qb + 1) * half], probs, preferred_element_type=F32)
                o_scr[pl.ds(pl.multiple_of(s * 128 + 64 * hh, 64), 64), cols] = (head_out * (1.0 / total)).astype(BF16)
        hidden = (0.5 * pre * (1.0 + lax.erf(pre * 0.7071067811865476))).astype(BF16)
        acc_scr[...] += jnp.dot(hidden, w_ref[s, 1024:1536, :], preferred_element_type=F32)
        return carry

    lax.fori_loop(0, 4, head_pair_and_mlp_part, 0, unroll=4)

    def out_rows(r, carry):
        rows = pl.ds(pl.multiple_of(r * half, half), half)
        w_out = w_ref[:, 384:512, :].reshape(width, width)
        heads = lax.dot_general(o_scr[:, rows], w_out, (((0,), (0,)), ((), ())), preferred_element_type=F32)
        x_ref[rows, :] = (acc_scr[rows, :] + heads).astype(BF16)
        return carry

    lax.fori_loop(0, 2, out_rows, 0, unroll=2)


def kernel(buf_ref, mb_ref, pos_ref, freq_ref, ln_attn, ln_mlp, w_qkv, w_out, w_up, w_down, emit_one, emit_two, final,
           w_all, xs, pos_scr, freq_scr, ln_scr, row_scr, lane_scr, m_scr, q_scr, k_scr, v_scr, o_scr, acc_scr,
           loc_sem, wloc_sem, ln_sem, xs_send, xs_recv, mb_send, mb_recv, y_recv, wz_send, wz_recv, wx_send, wx_recv,
           y_send, emit_recv, final_recv, column_sem):
    d, t, p = lax.axis_index("dp"), lax.axis_index("tp"), lax.axis_index("pp")
    emits = (emit_one, emit_two)
    second = 3 - 2 * lax.min(t, 1)
    outward = (2, second, 4 - second)

    def remote(src, dst, send, recv, dp=None, tp=None, pp=None):
        where = (d if dp is None else dp, t if tp is None else tp, p if pp is None else pp)
        return pltpu.make_async_remote_copy(src, dst, send, recv, device_id=where, device_id_type=MESH)

    def wait_bytes(ref, sem):
        pltpu.make_async_copy(ref, ref, sem).wait()

    def seq_rows(rank):
        return pl.ds(pl.multiple_of(rank * 128, 128), 128)

    def x_copy(i, o):
        to = lax.rem(t + o, 4)
        return remote(buf_ref.at[0, 8 * to + i], xs.at[0, i, seq_rows(t), :], xs_send, xs_recv.at[i, o - 1], tp=to)

    def x_arrived(i, o):
        src = lax.rem(t + 4 - o, 4)
        wait_bytes(xs.at[0, i, seq_rows(src), :], xs_recv.at[i, o - 1])

    def mb_copy(i, o):
        to = lax.rem(t + o, 4)
        return remote(mb_ref.at[8 * to + i], xs.at[1, i, seq_rows(t), :], mb_send, mb_recv.at[i, o - 1], tp=to)

    def mb_arrived(i, o):
        src = lax.rem(t + 4 - o, 4)
        wait_bytes(xs.at[1, i, seq_rows(src), :], mb_recv.at[i, o - 1])

    def x_local(i):
        return pltpu.make_async_copy(buf_ref.at[0, 8 * t + i], xs.at[0, i, seq_rows(t), :], loc_sem.at[0, i])

    def mb_local(i):
        return pltpu.make_async_copy(mb_ref.at[8 * t + i], xs.at[1, i, seq_rows(t), :], loc_sem.at[1, i])

    def send_x(i):
        for o in outward:
            x_copy(i, o).start()

    def half_rows(dp, piece):
        size = 256 * (piece + 1)
        return pl.ds(pl.multiple_of(512 * piece + dp * size, 256), size)

    def w_copy_z(s, piece, to, slot):
        rows = half_rows(d, piece)
        return remote(w_all.at[s, rows, :], w_all.at[s, rows, :], wz_send.at[slot, piece], wz_recv.at[s, piece], tp=to)

    def w_copy_x(s, piece):
        rows = half_rows(d, piece)
        return remote(w_all.at[s, rows, :], w_all.at[s, rows, :], wx_send.at[s, piece], wx_recv.at[s, piece], dp=1 - d)

    def relay(action):
        for hop in range(4):
            for piece in range(2):
                right_src, left_src = lax.max(t - hop, 0), lax.min(t + hop, 3)
                from_left, from_right = t >= hop, t + hop <= 3
                if hop:
                    for arrived, s in ((from_left, right_src), (from_right, left_src)):
                        @pl.when(arrived)
                        def _():
                            action("arrive", None, s, piece)
                if hop < 3:
                    @pl.when(jnp.logical_and(from_left, t < 3))
                    def _():
                        action("z", w_copy_z(right_src, piece, lax.min(t + 1, 3), 2 * hop), right_src, piece)

                    @pl.when(jnp.logical_and(from_right, t > 0))
                    def _():
                        action("z", w_copy_z(left_src, piece, lax.max(t - 1, 0), 2 * hop + 1), left_src, piece)
                if hop:
                    for arrived, s in ((from_left, right_src), (from_right, left_src)):
                        @pl.when(arrived)
                        def _():
                            action("x", w_copy_x(s, piece), s, piece)
            yield hop

    def start_or_wait(kind, copy, s, piece):
        if kind == "arrive":
            wait_bytes(w_all.at[s, half_rows(d, piece), :], wz_recv.at[s, piece])
        else:
            copy.start()

    def wait_sent(kind, copy, s, piece):
        if kind != "arrive":
            copy.wait_send()

    barrier = pltpu.get_barrier_semaphore()
    for o in (1, 2, 3):
        pl.semaphore_signal(barrier, inc=1, device_id=(d, lax.rem(t + o, 4), p), device_id_type=MESH)
        pl.semaphore_signal(barrier, inc=1, device_id=(d, t, lax.rem(p + o, 4)), device_id_type=MESH)
    pl.semaphore_signal(barrier, inc=1, device_id=(1 - d, t, p), device_id_type=MESH)

    own = []
    for head in range(2):
        for j, row in ((0, 0), (1, 256)):
            for side in range(2):
                own.append((w_qkv.at[0, head, j, pl.ds(32 * side, 32), :], row + 64 * side + 32 * head, 32))
        own.append((w_qkv.at[0, head, 2], 128 + 64 * head, 64))
    own += [(w_out.at[0], 384, 128), (w_up.at[0], 512, 512), (w_down.at[0], 1024, 512)]
    for src, row, size in own:
        pltpu.make_async_copy(src, w_all.at[t, pl.ds(row, size), :], wloc_sem).start()
    small = [pltpu.make_async_copy(ln_attn.at[0], ln_scr.at[0], ln_sem.at[0]), pltpu.make_async_copy(ln_mlp.at[0], ln_scr.at[1], ln_sem.at[1]),
             pltpu.make_async_copy(pos_ref, pos_scr, ln_sem.at[2]), pltpu.make_async_copy(freq_ref, freq_scr, ln_sem.at[3])]
    for copy in small:
        copy.start()
    for i in range(8):
        x_local(i).start()

    pl.semaphore_wait(barrier, 7)

    send_x(0)
    for o in (1, 2, 3):
        pl.semaphore_signal(column_sem, inc=1, device_id=(d, lax.rem(t + o, 4), p), device_id_type=MESH)
    wait_bytes(w_all.at[t], wloc_sem)
    for hop in relay(start_or_wait):
        for i in ((), (1, 2), (3, 4), (5, 6, 7))[hop]:
            send_x(i)

    @pl.when(p == 0)
    def _():
        def body(i, carry):
            mb_local(i).start()
            for o in outward:
                mb_copy(i, o).start()
            return carry
        lax.fori_loop(0, 8, body, 0)

        def zero_body(i, carry):
            final[0, i] = jnp.zeros(final.shape[2:], BF16)
            return carry
        lax.fori_loop(0, 32, zero_body, 0)

    for copy in small:
        copy.wait()
    row_scr[0], row_scr[1], lane_scr[0], lane_scr[1] = rope_angles(pos_scr[...], freq_scr[...])
    for o in (1, 2, 3):
        src = lax.rem(t + 4 - o, 4)
        for piece in range(2):
            wait_bytes(w_all.at[src, half_rows(1 - d, piece), :], wx_recv.at[src, piece])

    def emit_copy(tick, i, o, qq):
        to = lax.rem(t + o, 4)
        q = lax.rem(3 + qq, 4)
        src = xs.at[tick, i, seq_rows(to), seq_rows(q)]
        dst = emits[tick].at[8 * t + i]
        return remote(src, dst, y_send.at[tick, i], emit_recv.at[tick, o], tp=to, pp=q)

    def tick_body(tick):
        def step(i, carry):
            if tick == 0:
                x_local(i).wait()
                for o in (1, 2, 3):
                    x_arrived(i, o)
            else:
                @pl.when(p == 0)
                def _():
                    mb_local(i).wait()
                    for o in (1, 2, 3):
                        mb_arrived(i, o)

                @pl.when(p > 0)
                def _():
                    wait_bytes(xs.at[1, i], y_recv.at[i])
            layer(xs.at[tick, i], w_all, ln_scr, row_scr, lane_scr, m_scr, q_scr, k_scr, v_scr, o_scr, acc_scr)

            @pl.when(p < 3)
            def _():
                nxt = lax.min(p + 1, 3)
                if tick == 0:
                    remote(xs.at[0, i], xs.at[1, i], y_send.at[0, i], y_recv.at[i], pp=nxt).start()
                else:
                    for o in outward + (0,):
                        to = lax.rem(t + o, 4)
                        remote(xs.at[1, i, seq_rows(to), :], final.at[0, 8 * t + i], y_send.at[1, i], final_recv.at[o],
                               tp=to, pp=nxt).start()

            @pl.when(p == 3)
            def _():
                for o in outward + (0,):
                    for qq in (1, 2, 3, 0):
                        if isinstance(o, int) and o == 0 and qq == 0:
                            emits[tick][8 * t + i] = xs[tick, i, seq_rows(t), 384:512]
                        else:
                            emit_copy(tick, i, o, qq).start()
            return carry
        lax.fori_loop(0, 8, step, 0)

    pl.semaphore_wait(column_sem, 3)
    tick_body(0)
    tick_body(1)

    wait_bytes(buf_ref.at[0, 0:24], xs_send)
    for _ in relay(wait_sent):
        pass

    @pl.when(p == 0)
    def _():
        wait_bytes(mb_ref.at[0:24], mb_send)

    @pl.when(p > 0)
    def _():
        for o in range(4):
            src = lax.rem(t + 4 - o, 4)
            wait_bytes(final.at[0, pl.ds(8 * src, 8)], final_recv.at[o])

    for tick in range(2):
        for o in range(4):
            @pl.when(jnp.logical_or(p < 3, o > 0))
            def _():
                wait_bytes(emits[tick].at[pl.ds(8 * lax.rem(t + 4 - o, 4), 8)], emit_recv.at[tick, o])

        def sent(i, carry):
            @pl.when(p < 3)
            def _():
                wait_bytes(xs.at[tick, i], y_send.at[tick, i])

            @pl.when(p == 3)
            def _():
                wait_bytes(emits[tick].at[0:15], y_send.at[tick, i])
            return carry
        lax.fori_loop(0, 8, sent, 0)


def unload(*refs):
    copies = []
    for j in range(3):
        source, target = (refs[j].at[0], refs[3 + j].at[0]) if j == 2 else (refs[j], refs[3 + j])
        step = source.shape[0] // (4 if j == 2 else 1)
        for k in range(0, source.shape[0], step):
            copies.append(pltpu.make_async_copy(source.at[pl.ds(k, step)], target.at[pl.ds(k, step)], refs[6].at[len(copies)]))
    for copy in copies:
        copy.start()
    for copy in copies:
        copy.wait()


def solution(mesh):
    def body(stage_buf, new_mb, positions, ln_attn, ln_mlp, w_qkv, w_out, w_up, w_down):
        head_dim = w_qkv.shape[3]
        inv_freq = 1.0 / np.power(np.float32(ROPE_BASE), np.arange(0, head_dim, 2).astype(np.float32) / np.float32(head_dim))
        inv_freq = jnp.asarray(np.tile(inv_freq.astype(np.float32), 4)[None])
        batch, rows, width = new_mb.shape
        seq = 4 * rows
        emit_shape = jax.ShapeDtypeStruct((batch, rows, width // 4), BF16)
        hbm = pl.BlockSpec(memory_space=pl.ANY)
        vmem = pl.BlockSpec(memory_space=pltpu.VMEM)
        dma = pltpu.SemaphoreType.DMA
        shapes = (emit_shape, emit_shape, jax.ShapeDtypeStruct(stage_buf.shape, BF16))
        landed = pl.pallas_call(
            kernel,
            out_shape=tuple(pltpu.VMEM(sh.shape, BF16) for sh in shapes),
            in_specs=[hbm, hbm, hbm, hbm, hbm, hbm, hbm, hbm, hbm, hbm],
            out_specs=(vmem, vmem, vmem),
            scratch_shapes=[
                pltpu.VMEM((4, 1536, width), BF16),
                pltpu.VMEM((2, batch // 4, seq, width), BF16),
                pltpu.VMEM((1, seq), jnp.int32),
                pltpu.VMEM((1, 128), F32),
                pltpu.VMEM((2, 2, width), F32),
                pltpu.VMEM((2, seq, 128), F32),
                pltpu.VMEM((2, 64, seq), F32),
                pltpu.VMEM((seq, width), BF16),
                pltpu.VMEM((4, 128, seq), BF16),
                pltpu.VMEM((4, seq, 128), BF16),
                pltpu.VMEM((4, 128, seq), BF16),
                pltpu.VMEM((seq, width), BF16),
                pltpu.VMEM((seq, width), F32),
                dma((2, 8)), dma, dma((4,)), dma, dma((8, 3)), dma, dma((8, 3)), dma((8,)),
                dma((6, 2)), dma((4, 2)), dma((4, 2)), dma((4, 2)),
                dma((2, 8)), dma((2, 4)), dma((4,)), pltpu.SemaphoreType.REGULAR,
            ],
            compiler_params=pltpu.CompilerParams(has_side_effects=True, collective_id=0, vmem_limit_bytes=57 * 1024 * 1024),
            cost_estimate=pl.CostEstimate(flops=60_000_000_000, bytes_accessed=40_000_000, transcendentals=50_000_000),
        )(stage_buf, new_mb, positions[None, :], inv_freq, ln_attn, ln_mlp, w_qkv, w_out, w_up, w_down)
        landed = [pltpu.with_memory_space_constraint(x, pltpu.VMEM) for x in landed]
        return pl.pallas_call(
            unload,
            out_shape=shapes,
            in_specs=[vmem, vmem, vmem],
            out_specs=(hbm, hbm, hbm),
            scratch_shapes=[dma((6,))],
            compiler_params=pltpu.CompilerParams(vmem_limit_bytes=1024 * 1024),
            cost_estimate=pl.CostEstimate(flops=1_000_000, bytes_accessed=12_000_000, transcendentals=0),
        )(*landed)

    act_spec = P("dp", "tp", None)
    buf_spec = P("pp", "dp", "tp", None)
    emit_spec = P("dp", "tp", "pp")
    stack_spec = P("pp", None, None)
    return jax.shard_map(body, mesh=mesh, in_specs=(buf_spec, act_spec, P(None), stack_spec, stack_spec, P("pp", "tp", None, None, None), P("pp", "tp", None), P("pp", None, "tp"), P("pp", "tp", None)), out_specs=(emit_spec, emit_spec, buf_spec), check_vma=False)
```
